1024 devices in a mesh: dp: 64 (over y, z_lo, core), tensor: 16 (over x, z_hi).
Axes of the slice: x: 4, y: 4, z: 32 (z_hi: 4, z_lo: 8; z = z_hi * 8 + z_lo), core: 2. Of those that a mesh axis runs over, the one named last changes fastest.
Arguments:
- hidden_in: bfloat16 [64, 128, 16384], P('dp'), may hold values from -16 to 16
- value_weight: bfloat16 [16384, 1024], P(None, 'tensor'), may hold values from -0.046875 to 0.046875
- queries: bfloat16 [64, 128, 16384], P('dp', None, 'tensor'), may hold values from -4 to 4
- key_rows: bfloat16 [64, 128, 1024], P('dp', None, 'tensor'), may hold values from -4 to 4
- attention_out: bfloat16 [64, 128, 16384], P('dp', None, 'tensor'), may hold values from -4 to 4
- output_grad: bfloat16 [64, 128, 16384], P('dp', None, 'tensor'), may hold values from -6 to 6
- log_normalizer: float32 [64, 128, 128], P('dp', None, 'tensor'), may hold values from 1 to 5
- document_ids: int32 [64, 128], P('dp'), may hold values from 0 to 3, never falling along the last dimension, each value on 1 to 64 neighbouring positions
Outputs:
- query_grad: bfloat16 [64, 128, 16384], P('dp', None, 'tensor')
- key_grad: bfloat16 [64, 128, 1024], P('dp', None, 'tensor')
- input_grad: bfloat16 [64, 128, 16384], P('dp', 'tensor')
- value_weight_grad: float32 [16384, 1024], P('dp', 'tensor')
The draws below stay inside these ranges and needn't reach their ends.
Inputs may be any that keep to these rules, and one draw needn't show every extreme that they name: `document_ids`: within one group the ids never fall; all 4 documents occur, each of 1 to 64 tokens.
All inputs are finite; a program needn't handle non-finite values.
Results may differ from the reference program's by a relative error of at most 0.014.
Values may be sent and summed in bfloat16 or wider, within the bound.
A program may use at most 64 MiB of HBM per device.

```python
import math
from functools import partial
import jax
import jax.numpy as jnp
import numpy as np
from jax import lax

D = 16384
HD = 128
GROUP = 16
TOK_DEV = 128
DOCS = 4
QHEADS = 128
KVH = 8
GROUPS = 64


def raised(values, own_key, source, target, shards_of, factor):
    owner, partner = [(jnp.arange(values.shape[dim]) // (values.shape[dim] // shards_of)).reshape([-1 if axis == dim else 1 for axis in range(values.ndim)]) for dim in (source, target)]
    chosen = jax.random.permutation(own_key, shards_of)[partner]
    strong = (owner == chosen) | (owner == (partner + shards_of // 2) % shards_of)
    return jnp.where(strong, factor * values, values)


def block_scale(stream_key, shape, pieces, smallest, high):
    level = 1.0
    for dim, parts in pieces:
        draws = jax.random.uniform(jax.random.fold_in(jax.random.fold_in(stream_key, 6), dim), (parts,), jnp.float32, smallest / len(pieces), high / len(pieces))
        level = level * jnp.repeat(jnp.exp(draws), shape[dim] // parts).reshape((-1,) + (1,) * (len(shape) - 1 - dim))
    return level


def profile(count, total, reach, lean):
    loads = [(1 << 20) // math.isqrt(grade ** lean) + 1 for grade in range(2, count + 1)]
    spare, counts = total - reach - (count - 1), [1] * (count - 1)
    while spare > 0:
        candidates = [i for i in range(count - 1) if counts[i] < reach]
        whole, budget = sum([loads[i] for i in candidates]), spare
        for i in candidates:
            addition = min(reach - counts[i], max(1, budget * loads[i] // whole), spare)
            counts[i] = counts[i] + addition
            spare = spare - addition
    return np.array([reach] + counts)


def uneven_parts(stream_key, amount, total, limit, skew):
    if amount == 2:
        one = jax.random.randint(stream_key, (), max(1, total - limit), min(limit, total - 1) + 1)
        return jnp.stack([one, total - one])
    sizes = jnp.asarray(profile(amount, total, limit, skew), jnp.int32)
    twos = (amount - 1) // 2
    source_of, sink = sizes[1:1 + 2 * twos:2], sizes[2:2 + 2 * twos:2]
    slack = jnp.minimum(source_of - 1, limit - sink)
    moved = jax.random.randint(jax.random.fold_in(stream_key, 1), (twos,), 0, 1 << 20) % (slack + 1)
    sizes = sizes.at[1:1 + 2 * twos:2].set(source_of - moved).at[2:2 + 2 * twos:2].set(sink + moved)
    return sizes[jax.random.permutation(jax.random.fold_in(stream_key, 2), amount)]


def gaussian(rng, extent, scale, reach, split=(), held_as=jnp.bfloat16):
    result = scale * jax.random.normal(rng, extent, jnp.float32)
    if split:
        result = result * block_scale(rng, extent, split, -0.22, 0.18)
    return jnp.clip(result, -reach, reach).astype(held_as)


def heavy_noise(key, dims, deviation, limit, split, heavy, kind=jnp.bfloat16):
    values = deviation * jax.random.normal(key, dims, jnp.float32)
    if split:
        values = values * block_scale(key, dims, split, -0.22, 0.18)
    return jnp.clip(raised(values, jax.random.fold_in(key, 3), *heavy), -limit, limit).astype(kind)


def setup_inputs(seed: int = 0) -> dict:
    keys = jax.random.split(jax.random.key(seed), 9)
    hidden_in = heavy_noise(keys[0], (GROUPS, TOK_DEV, D), 1.0, 16.0, ((0, 64),), (0, 2, 64, 4.0))
    value_weight = gaussian(keys[1], (D, KVH * HD), D ** -0.5, 0.046875, ((1, 16),))
    queries = gaussian(keys[2], (GROUPS, TOK_DEV, QHEADS * HD), 1.0, 4.0, ((0, 64), (2, 16)))
    key_rows = gaussian(keys[3], (GROUPS, TOK_DEV, KVH * HD), 1.0, 4.0, ((0, 64), (2, 16)))
    attention_out = gaussian(keys[4], (GROUPS, TOK_DEV, QHEADS * HD), 0.5, 4.0, ((0, 64), (2, 16)))
    output_grad = heavy_noise(keys[5], (GROUPS, TOK_DEV, QHEADS * HD), 1.0, 6.0, ((0, 64), (2, 16)), (2, 1, 16, 2.0))
    log_normalizer = jnp.clip(1.0 + 4.0 * jax.random.uniform(keys[6], (GROUPS, TOK_DEV, QHEADS), jnp.float32) ** block_scale(keys[6], (GROUPS, TOK_DEV, QHEADS), ((0, 64), (2, 16)), -0.2, 0.2), 1.0, 5.0)
    document_ids = jax.vmap(lambda own: jnp.searchsorted(jnp.cumsum(uneven_parts(own, DOCS, TOK_DEV, TOK_DEV // 2, 1)), jnp.arange(TOK_DEV), side="right"))(jax.random.split(keys[7], GROUPS)).reshape((GROUPS, TOK_DEV)).astype(jnp.int32)
    return {"hidden_in": hidden_in, "value_weight": value_weight, "queries": queries, "key_rows": key_rows, "attention_out": attention_out, "output_grad": output_grad, "log_normalizer": log_normalizer, "document_ids": document_ids}


def rounded(array):
    return lax.optimization_barrier(array.astype(jnp.bfloat16)).astype(jnp.float32)

def group_backward(value_weight, operands):
    hidden_in, queries, key_rows, attention_out, output_grad, log_normalizer, document_ids = operands
    tokens = hidden_in.shape[0]
    score_scale = 1.0 / math.sqrt(HD)
    values = jnp.dot(hidden_in, value_weight, preferred_element_type=jnp.float32).astype(jnp.bfloat16)
    query_heads = queries.astype(jnp.float32).reshape(tokens, KVH, GROUP, HD)
    key_heads = key_rows.astype(jnp.float32).reshape(tokens, KVH, HD)
    value_heads = values.astype(jnp.float32).reshape(tokens, KVH, HD)
    out_heads = attention_out.astype(jnp.float32).reshape(tokens, KVH, GROUP, HD)
    grad_heads = output_grad.astype(jnp.float32).reshape(tokens, KVH, GROUP, HD)
    normalizers = jnp.transpose(log_normalizer.reshape(tokens, KVH, GROUP), (1, 2, 0))[..., None]
    position = jnp.arange(tokens, dtype=jnp.int32)
    allowed = (position[None, :] <= position[:, None]) & (document_ids[:, None] == document_ids[None, :])
    scores = jnp.einsum('tcgd,scd->cgts', query_heads, key_heads) * score_scale
    probabilities = jnp.where(allowed, jnp.exp(scores - normalizers), 0.0)
    probs_low = rounded(probabilities)
    value_sum = jnp.einsum('cgts,tcgd->scd', probs_low, grad_heads)
    row_dots = jnp.einsum('tcgd,tcgd->cgt', grad_heads, out_heads)
    prob_grad = jnp.einsum('tcgd,scd->cgts', grad_heads, value_heads)
    score_grad = rounded(probabilities * (prob_grad - row_dots[..., None]) * score_scale)
    query_grad = jnp.einsum('cgts,scd->tcgd', score_grad, key_heads).astype(jnp.bfloat16)
    key_grad = jnp.einsum('cgts,tcgd->scd', score_grad, query_heads).astype(jnp.bfloat16)
    value_grad = value_sum.astype(jnp.bfloat16).reshape(tokens, KVH * HD)
    block_width = HD // 2

    def add_block(summed, block_index):
        offset = block_index * block_width
        row_block = lax.dynamic_slice_in_dim(value_grad, offset, block_width, 1)
        col_block = lax.dynamic_slice_in_dim(value_weight, offset, block_width, 1)
        product = lax.dot_general(row_block, col_block, (((1,), (1,)), ((), ())), preferred_element_type=jnp.float32)
        return (summed + rounded(product), None)
    start_sum = jnp.zeros((tokens, value_weight.shape[0]), jnp.float32)
    input_sum, unused = lax.scan(add_block, start_sum, jnp.arange(2 * KVH, dtype=jnp.int32))
    return (query_grad.reshape(tokens, KVH * GROUP * HD), key_grad.reshape(tokens, KVH * HD), input_sum.astype(jnp.bfloat16), value_grad)

def reference(hidden_in, value_weight, queries, key_rows, attention_out, output_grad, log_normalizer, document_ids):
    results = lax.map(partial(group_backward, value_weight), (hidden_in, queries, key_rows, attention_out, output_grad, log_normalizer, document_ids))
    query_grad, key_grad, input_grad, value_grad = results
    flat_inputs = hidden_in.reshape(-1, hidden_in.shape[2])
    flat_grads = value_grad.reshape(-1, value_grad.shape[2])
    value_weight_grad = lax.dot_general(flat_inputs, flat_grads, (((0,), (0,)), ((), ())), preferred_element_type=jnp.float32)
    return (query_grad, key_grad, input_grad, value_weight_grad)
```

```python
import functools
import math

import jax
import jax.numpy as jnp
from jax import lax
from jax.experimental import pallas as pl
from jax.experimental.pallas import tpu as pltpu
from jax.sharding import Mesh
from jax.sharding import PartitionSpec as P

DP = ("y", "w", "c")
TENSOR = ("x", "v")
BF16 = jnp.bfloat16
F32 = jnp.float32


def dot(a, b, da, db):
    return lax.dot_general(a, b, (((da,), (db,)), ((), ())), preferred_element_type=F32)


def pack(a):
    rows = a.shape[0] // 2
    return jnp.concatenate([a[:rows], a[rows:]], axis=1)


def unpack(a):
    width = a.shape[1] // 2
    return jnp.concatenate([a[:, :width], a[:, width:]], axis=0)


def kernel(
    sizes,
    hidden_hbm,
    weight_hbm,
    query_hbm,
    key_hbm,
    out_hbm,
    grad_hbm,
    norm_ref,
    docs_ref,
    qgrad_ref,
    kgrad_ref,
    igrad_ref,
    wgrad_ref,
    hidden,
    weight,
    query,
    key_half,
    attn_out,
    grad,
    weight_rows,
    weight_cols,
    key_send,
    key_recv,
    val_send,
    val_recv,
    keys,
    values,
    probs,
    half_send,
    half_recv,
    kpart_send,
    kpart_recv,
    part_send,
    part_recv,
    plane_grads,
    plane_weights,
    out_send,
    out_recv,
    keep,
    core_send,
    core_recv,
    y_send,
    y_recv,
    w_send,
    w_recv,
    local_sem,
    hidden_sem,
    rows_sem,
    pair_send,
    pair_recv,
    x_sems,
    v_send,
    v_recv,
    part_ssem,
    part_rsem,
    chain_send,
    chain_recv,
    plane_sems,
    core_ssem,
    core_rsem,
    y_ssem,
    y_rsem,
    w_sems,
):
    NX, NY, NW, NC, NV = sizes
    T, D = hidden.shape
    half = key_half.shape[1]
    width = 2 * half
    heads = norm_ref.shape[1]
    scale = 1.0 / math.sqrt(width)
    NS = NX * NY * NC
    DS = D // NS
    DB = DS // 2
    RG = NW // 2
    R = half // RG
    TR = T // (NX * NV)
    TV = T // NV
    BD = D // (NY * NW * NC)
    x, y, w, c, v = (lax.axis_index(name) for name in ("x", "y", "w", "c", "v"))
    me = (x * NY + y) * NC + c
    member = v % 2
    lower = member == 0
    depth_half, row_group = w // RG, w % RG

    def plane(i):
        dx, dy, dc = i // (NY * NC), (i // NC) % NY, i % NC
        px, py, pc = (x + dx) % NX, (y + dy) % NY, (c + dc) % NC
        return {"x": px, "y": py, "c": pc}, (px * NY + py) * NC + pc

    position = v * NW + w
    after, before = (position + 1) % (NV * NW), (position + NV * NW - 1) % (NV * NW)
    up = {"v": after // NW, "w": after % NW}
    down = {"v": before // NW, "w": before % NW}
    pair = {"v": v + 1 - 2 * member}

    def remote(src, dst, send, recv, device):
        return pltpu.make_async_remote_copy(
            src_ref=src,
            dst_ref=dst,
            send_sem=send,
            recv_sem=recv,
            device_id=device,
            device_id_type=pl.DeviceIdType.MESH,
        )

    def wait_for(ref, sem):
        pltpu.make_async_copy(ref, ref, sem).wait()

    key_copy = pltpu.make_async_copy(key_hbm, key_half, local_sem.at[0])
    key_copy.start()
    row_copies = []
    for i in range(NX):
        start = ((i * NY + y) * NC + c) * DS + depth_half * DB
        row_copies.append(
            pltpu.make_async_copy(
                weight_hbm.at[pl.ds(pl.multiple_of(start, DB), DB)],
                weight_rows.at[i],
                rows_sem.at[i],
            )
        )
        row_copies[-1].start()
    weight_copy = pltpu.make_async_copy(weight_hbm, weight, local_sem.at[1])
    weight_copy.start()
    HC = D // 4
    hidden_copies = [
        pltpu.make_async_copy(
            hidden_hbm.at[:, pl.ds(i * HC, HC)], hidden.at[:, pl.ds(i * HC, HC)], hidden_sem.at[i]
        )
        for i in range(4)
    ]
    for copy in hidden_copies:
        copy.start()
    query_copy = pltpu.make_async_copy(query_hbm, query, local_sem.at[2])
    grad_copy = pltpu.make_async_copy(grad_hbm, grad, local_sem.at[3])
    out_copy = pltpu.make_async_copy(out_hbm, attn_out, local_sem.at[4])
    for copy in (query_copy, grad_copy, out_copy):
        copy.start()

    barrier = pltpu.get_barrier_semaphore()

    def greet(device):
        pl.semaphore_signal(
            barrier, inc=1, device_id=device, device_id_type=pl.DeviceIdType.MESH
        )

    greet({"v": (v + 1) % NV})
    greet({"v": (v + NV - 1) % NV})
    greet(up)
    greet(down)

    def greet_plane(i, carry):
        greet(plane(i)[0])
        return carry

    lax.fori_loop(1, NS, greet_plane, 0)

    def greet_line(i, carry):
        greet({"w": (w + i) % NW})
        return carry

    lax.fori_loop(1, NW, greet_line, 0)

    key_copy.wait()
    own_key = key_half[...].astype(F32)
    key_send[...] = pack(own_key).astype(BF16)
    for copy in row_copies:
        copy.wait()
    for i in range(0, NX, 2):
        both = jnp.concatenate(
            [weight_rows[i].astype(F32), weight_rows[i + 1].astype(F32)], axis=1
        ).T
        weight_cols[i] = both[:half].astype(BF16)
        weight_cols[i + 1] = both[half:].astype(BF16)

    weight_copy.wait()
    CK = 1024
    total = jnp.zeros((T, half), F32)
    for i in range(4):
        hidden_copies[i].wait()

        def add_values(k, acc, base=i * HC):
            at = pl.multiple_of(base + k * CK, CK)
            return acc + dot(hidden[:, pl.ds(at, CK)], weight[pl.ds(at, CK), :], 1, 0)

        total = lax.fori_loop(0, HC // CK, add_values, total)
    own_value = total.astype(BF16).astype(F32)
    val_send[...] = pack(own_value).astype(BF16)

    pl.semaphore_wait(barrier, 4 + (NS - 1) + (NW - 1))

    key_exchange = remote(key_send, key_recv, pair_send.at[0], pair_recv.at[0], pair)
    key_exchange.start()
    own_rows = pl.ds(pl.multiple_of(row_group * R, R), R)
    for i in range(1, NX):
        to = (x + i) % NX
        remote(
            weight_cols.at[to, own_rows],
            plane_weights.at[w, v, x],
            x_sems.at[0],
            x_sems.at[1],
            {"x": to},
        ).start()
    own_copy = pltpu.make_async_copy(
        weight_cols.at[x, own_rows], plane_weights.at[w, v, x], local_sem.at[5]
    )
    own_copy.start()
    value_exchange = remote(val_send, val_recv, pair_send.at[1], pair_recv.at[1], pair)
    value_exchange.start()

    own_copy.wait()
    wait_for(plane_weights.at[w, v, pl.ds(0, NX - 1)], x_sems.at[1])

    def weights_to(j):
        return remote(
            plane_weights.at[w, v],
            plane_weights.at[w, v],
            v_send.at[j],
            v_recv.at[j],
            {"v": (v + j) % NV},
        )

    weights_to(1).start()
    weights_to(3).start()

    query_copy.wait()
    grad_copy.wait()
    rows = lax.broadcasted_iota(jnp.int32, (T, T), 0)
    columns = lax.broadcasted_iota(jnp.int32, (T, T), 1)
    documents = jnp.broadcast_to(docs_ref[...].astype(F32), (T, T))
    allowed = (columns <= rows) & (documents == documents.T)

    key_exchange.wait_recv()
    other_key = unpack(key_recv[...].astype(F32))
    keys[...] = jnp.concatenate(
        [jnp.where(lower, own_key, other_key), jnp.where(lower, other_key, own_key)], axis=1
    ).astype(BF16)
    weights_to(2).start()

    value_part = jnp.zeros((T, width), F32)
    for h in range(heads):
        lanes = pl.ds(h * width, width)
        scores = dot(query[:, lanes], keys[...], 1, 1) * scale
        prob = jnp.where(allowed, jnp.exp(scores - norm_ref[:, h : h + 1]), 0.0)
        probs[h] = prob
        value_part = value_part + dot(prob.astype(BF16), grad[:, lanes], 0, 0)

    own_half = jnp.where(lower, value_part[:, :half], value_part[:, half:])
    other_half = jnp.where(lower, value_part[:, half:], value_part[:, :half])
    half_send[...] = pack(other_half).astype(BF16)
    half_exchange = remote(half_send, half_recv, pair_send.at[2], pair_recv.at[2], pair)
    half_exchange.start()
    by_token = value_part.reshape(NX, NV, TR, width)
    for i in range(NV):
        part_send[i] = by_token[:, i].reshape(TV, width).astype(BF16)

    def part_to(j):
        to = (v + j) % NV
        return remote(
            part_send.at[to], part_recv.at[v], part_ssem.at[j], part_rsem.at[j], {"v": to}
        )

    for j in (2, 1, 3):
        part_to(j).start()
    part_recv[v] = part_send[v]

    out_copy.wait()
    value_exchange.wait_recv()
    other_value = unpack(val_recv[...].astype(F32))
    values[...] = jnp.concatenate(
        [jnp.where(lower, own_value, other_value), jnp.where(lower, other_value, own_value)], axis=1
    ).astype(BF16)
    key_part = jnp.zeros((T, width), F32)
    for h in range(heads):
        lanes = pl.ds(h * width, width)
        head_grad = grad[:, lanes]
        row_dots = jnp.sum(
            head_grad.astype(F32) * attn_out[:, lanes].astype(F32), axis=1, keepdims=True
        )
        prob_grad = dot(head_grad, values[...], 1, 1)
        score_grad = (probs[h] * (prob_grad - row_dots) * scale).astype(BF16)
        qgrad_ref[:, lanes] = dot(score_grad, keys[...], 1, 0).astype(BF16)
        key_part = key_part + dot(score_grad, query[:, lanes], 0, 0)
    own_kpart = jnp.where(lower, key_part[:, :half], key_part[:, half:])
    other_kpart = jnp.where(lower, key_part[:, half:], key_part[:, :half])
    kpart_send[...] = pack(other_kpart).astype(BF16)
    kpart_exchange = remote(kpart_send, kpart_recv, pair_send.at[3], pair_recv.at[3], pair)
    kpart_exchange.start()

    half_exchange.wait_recv()
    value_grad = own_half + unpack(half_recv[...].astype(F32))
    value_grad_t = jnp.concatenate([value_grad, value_grad], axis=1).T[:half].astype(BF16)

    def core_copy(off):
        return remote(
            core_send.at[off],
            core_recv.at[off],
            core_ssem.at[off],
            core_rsem.at[off],
            {"c": 1 - c},
        )

    def make_blocks(off, carry):
        to_w = (w + off) % NW
        for j in range(NY):
            block = (((y + j) % NY) * NW + to_w) * NC
            own = pl.multiple_of((block + c) * BD, BD)
            other = pl.multiple_of((block + 1 - c) * BD, BD)
            core_send[off, j] = dot(value_grad_t, hidden[:, pl.ds(other, BD)], 1, 0).astype(BF16)
            keep[off, j] = dot(value_grad_t, hidden[:, pl.ds(own, BD)], 1, 0)
        core_copy(off).start()
        return carry

    lax.fori_loop(0, NW, make_blocks, 0)

    def send_y(off, carry):
        core_copy(off).wait_recv()
        for j in range(1, NY):
            y_send[off, j - 1] = (keep[off, j] + core_recv[off, j].astype(F32)).astype(BF16)
            remote(
                y_send.at[off, j - 1],
                y_recv.at[off, j - 1],
                y_ssem,
                y_rsem.at[off],
                {"y": (y + j) % NY},
            ).start()
        keep[off, 0] = keep[off, 0] + core_recv[off, 0].astype(F32)
        return carry

    lax.fori_loop(0, NW, send_y, 0)

    for j in (1, 3, 2):
        part_to(j).wait_recv()
    own_tokens = jnp.concatenate(
        [
            part_recv[2 * i].astype(F32) + part_recv[2 * i + 1].astype(F32)
            for i in range(NV // 2)
        ],
        axis=1,
    )
    plane_grads[me] = own_tokens.astype(BF16)

    def send_grads(i, carry):
        remote(
            plane_grads.at[me], plane_grads.at[me], plane_sems.at[0], plane_sems.at[1], plane(i)[0]
        ).start()
        return carry

    lax.fori_loop(1, NS, send_grads, 0)

    for j in (1, 3, 2):
        weights_to(j).wait_recv()
    UP, DOWN = NW // 2, (NW - 1) // 2

    def chain_up(k):
        block = plane_weights.at[(w + NW - k) % NW]
        return remote(block, block, chain_send.at[0, k], chain_recv.at[0, k], up)

    def chain_down(k):
        block = plane_weights.at[(w + k) % NW]
        return remote(block, block, chain_send.at[1, k], chain_recv.at[1, k], down)

    def send_w(off):
        wait_for(y_recv.at[off], y_rsem.at[off])
        summed = keep[off, 0]
        for j in range(NY - 1):
            summed = summed + y_recv[off, j].astype(F32)
        if off == 0:
            keep[0, 0] = summed
            return
        w_send[off - 1] = summed.astype(BF16)
        remote(
            w_send.at[off - 1],
            w_recv.at[off - 1],
            w_sems.at[0],
            w_sems.at[1],
            {"w": (w + off) % NW},
        ).start()

    chain_up(0).start()
    if DOWN:
        chain_down(0).start()
    pending = list(range(1, NW)) + [0]
    share = -(-NW // UP)
    for k in range(UP):
        for off in pending[k * share : (k + 1) * share]:
            send_w(off)
        chain_up(k).wait_recv()
        if k + 1 < UP:
            chain_up(k + 1).start()
        if k < DOWN:
            chain_down(k).wait_recv()
            if k + 1 < DOWN:
                chain_down(k + 1).start()

    wait_for(plane_grads.at[pl.ds(0, NS - 1)], plane_sems.at[1])
    NG = NY * NC
    pieces = []
    for d in range(2):
        acc = jnp.zeros((NG * TV, DB), F32)
        for i in range(NX):
            left = plane_grads[i * NG : (i + 1) * NG].reshape(NG * TV, NV * half)
            right = jnp.concatenate(
                [plane_weights[d * RG + g, k, i] for k in range(NV) for g in range(RG)], axis=0
            )
            acc = acc + dot(left, right, 1, 0)
        pieces.append(acc.reshape(NG, NX, TR, DB))
    for i in range(NX):
        out_send[i * NG : (i + 1) * NG] = jnp.concatenate(
            [pieces[0][:, i], pieces[1][:, i]], axis=1
        ).astype(BF16)

    def send_out(i, carry):
        device, slot = plane(i)
        remote(
            out_send.at[slot], out_recv.at[me], plane_sems.at[2], plane_sems.at[3], device
        ).start()
        return carry

    lax.fori_loop(1, NS, send_out, 0)
    out_recv[me] = out_send[me]

    kpart_exchange.wait_recv()
    kgrad_ref[...] = (own_kpart + unpack(kpart_recv[...].astype(F32))).astype(BF16)
    wait_for(w_recv, w_sems.at[1])
    summed = keep[0, 0]
    for off in range(NW - 1):
        summed = summed + w_recv[off].astype(F32)
    wgrad_ref[...] = summed
    wait_for(out_recv.at[pl.ds(0, NS - 1)], plane_sems.at[3])
    igrad_ref[...] = out_recv[...]

    for exchange in (key_exchange, value_exchange, half_exchange, kpart_exchange):
        exchange.wait_send()
    wait_for(plane_weights.at[w, v, pl.ds(0, NX - 1)], x_sems.at[0])
    for j in (1, 2, 3):
        weights_to(j).wait_send()
        part_to(j).wait_send()
    for k in range(UP):
        chain_up(k).wait_send()
    for k in range(DOWN):
        chain_down(k).wait_send()

    def core_sent(off, carry):
        core_copy(off).wait_send()
        return carry

    lax.fori_loop(0, NW, core_sent, 0)
    wait_for(y_send, y_ssem)
    wait_for(w_send, w_sems.at[0])
    wait_for(plane_grads.at[pl.ds(0, NS - 1)], plane_sems.at[0])
    wait_for(out_send.at[pl.ds(0, NS - 1)], plane_sems.at[2])


def per_device(
    sizes,
    hidden_in,
    value_weight,
    queries,
    key_rows,
    attention_out,
    output_grad,
    log_normalizer,
    document_ids,
):
    NX, NY, NW, NC, NV = sizes
    T, D = hidden_in.shape[1:]
    half = key_rows.shape[2]
    width = 2 * half
    heads = log_normalizer.shape[2]
    NS = NX * NY * NC
    DS = D // NS
    DB = DS // 2
    R = half // (NW // 2)
    TR = T // (NX * NV)
    TV = T // NV
    BD = D // (NY * NW * NC)
    packed = pltpu.VMEM((T // 2, 2 * half), BF16)
    dma = pltpu.SemaphoreType.DMA
    scratch = [
        pltpu.VMEM((T, D), BF16),
        pltpu.VMEM((D, half), BF16),
        pltpu.VMEM((T, heads * width), BF16),
        pltpu.VMEM((T, half), BF16),
        pltpu.VMEM((T, heads * width), BF16),
        pltpu.VMEM((T, heads * width), BF16),
        pltpu.VMEM((NX, DB, half), BF16),
        pltpu.VMEM((NX, half, DB), BF16),
        packed,
        packed,
        packed,
        packed,
        pltpu.VMEM((T, width), BF16),
        pltpu.VMEM((T, width), BF16),
        pltpu.VMEM((heads, T, T), F32),
        packed,
        packed,
        packed,
        packed,
        pltpu.VMEM((NV, TV, width), BF16),
        pltpu.VMEM((NV, TV, width), BF16),
        pltpu.VMEM((NS, TV, NV * half), BF16),
        pltpu.VMEM((NW, NV, NX, R, DB), BF16),
        pltpu.VMEM((NS, 2 * TR, DB), BF16),
        pltpu.VMEM((NS, 2 * TR, DB), BF16),
        pltpu.VMEM((NW, NY, half, BD), F32),
        pltpu.VMEM((NW, NY, half, BD), BF16),
        pltpu.VMEM((NW, NY, half, BD), BF16),
        pltpu.VMEM((NW, NY - 1, half, BD), BF16),
        pltpu.VMEM((NW, NY - 1, half, BD), BF16),
        pltpu.VMEM((NW - 1, half, BD), BF16),
        pltpu.VMEM((NW - 1, half, BD), BF16),
        dma((6,)),
        dma((4,)),
        dma((NX,)),
        dma((4,)),
        dma((4,)),
        dma((2,)),
        dma((NV,)),
        dma((NV,)),
        dma((NV,)),
        dma((NV,)),
        dma((2, NW)),
        dma((2, NW)),
        dma((4,)),
        dma((NW,)),
        dma((NW,)),
        dma,
        dma((NW,)),
        dma((2,)),
    ]
    anywhere = pl.BlockSpec(memory_space=pl.ANY)
    vmem = pl.BlockSpec(memory_space=pltpu.VMEM)
    query_grad, key_grad, input_blocks, weight_grad = pl.pallas_call(
        functools.partial(kernel, sizes),
        out_shape=(
            jax.ShapeDtypeStruct((T, heads * width), BF16),
            jax.ShapeDtypeStruct((T, half), BF16),
            jax.ShapeDtypeStruct((NS, 2 * TR, DB), BF16),
            jax.ShapeDtypeStruct((half, BD), F32),
        ),
        in_specs=[anywhere] * 6 + [vmem] * 2,
        out_specs=(vmem,) * 4,
        scratch_shapes=scratch,
        compiler_params=pltpu.CompilerParams(
            collective_id=0, has_side_effects=True, vmem_limit_bytes=48 * 1024 * 1024
        ),
    )(
        hidden_in[0],
        value_weight,
        queries[0],
        key_rows[0],
        attention_out[0],
        output_grad[0],
        log_normalizer[0],
        document_ids,
    )
    input_grad = (
        input_blocks.reshape(NS, 2, TR, DB).transpose(2, 0, 1, 3).reshape(1, TR, D)
    )
    return query_grad[None], key_grad[None], input_grad, weight_grad.T


def over(finer):
    sizes = tuple(finer.shape[name] for name in ("x", "y", "w", "c", "v"))
    return jax.shard_map(
        functools.partial(per_device, sizes),
        mesh=finer,
        in_specs=(
            P(DP, None, None),
            P(None, TENSOR),
            P(DP, None, TENSOR),
            P(DP, None, TENSOR),
            P(DP, None, TENSOR),
            P(DP, None, TENSOR),
            P(DP, None, TENSOR),
            P(DP, None),
        ),
        out_specs=(P(DP, None, TENSOR), P(DP, None, TENSOR), P(DP, TENSOR, None), P(DP, TENSOR)),
        check_vma=False,
    )


def solution(mesh):
    return over(Mesh(mesh.devices.reshape(4, 8, 2, 4, 4), DP + TENSOR))
```

```python
import functools
import math

import jax
import jax.numpy as jnp
from jax import lax
from jax.experimental import pallas as pl
from jax.experimental.pallas import tpu as pltpu
from jax.sharding import Mesh
from jax.sharding import PartitionSpec as P

DP = ("y", "w", "c")
TENSOR = ("x", "v")
BF16 = jnp.bfloat16
F32 = jnp.float32


def dot(a, b, da, db):
    return lax.dot_general(a, b, (((da,), (db,)), ((), ())), preferred_element_type=F32)


def kernel(
    sizes,
    hidden_hbm,
    weight_hbm,
    query_hbm,
    key_hbm,
    out_hbm,
    grad_hbm,
    norm_hbm,
    docs_hbm,
    qgrad_ref,
    kgrad_ref,
    igrad_ref,
    wgrad_ref,
    norm_ref,
    docs_ref,
    hidden,
    weight,
    query,
    attn_out,
    grad,
    key_recv,
    val_recv,
    keys,
    values,
    probs,
    half_send,
    half_recv,
    kpart_send,
    kpart_recv,
    part_send,
    part_recv,
    plane_grads,
    plane_weights,
    out_send,
    out_recv,
    keep,
    core_send,
    core_recv,
    y_send,
    y_recv,
    w_send,
    w_recv,
    local_sem,
    hidden_sem,
    pair_send,
    pair_recv,
    x_sems,
    v_send,
    v_recv,
    part_ssem,
    part_rsem,
    chain_send,
    chain_recv,
    plane_sems,
    core_ssem,
    core_rsem,
    y_ssem,
    y_rsem,
    w_sems,
):
    NX, NY, NW, NC, NV = sizes
    T, D = hidden.shape
    half = weight.shape[0]
    width = 2 * half
    heads = norm_ref.shape[0]
    scale = 1.0 / math.sqrt(width)
    NS = NX * NY * NC
    DS = D // NS
    DB = DS // 2
    RG = NW // 2
    R = half // RG
    TR = T // (NX * NV)
    TV = T // NV
    BD = D // (NY * NW * NC)
    x, y, w, c, v = (lax.axis_index(name) for name in ("x", "y", "w", "c", "v"))
    me = (x * NY + y) * NC + c
    member = v % 2
    lower = member == 0
    depth_half, row_group = w // RG, w % RG

    def plane(i):
        dx, dy, dc = i // (NY * NC), (i // NC) % NY, i % NC
        px, py, pc = (x + dx) % NX, (y + dy) % NY, (c + dc) % NC
        return {"x": px, "y": py, "c": pc}, (px * NY + py) * NC + pc

    position = v * NW + w
    after, before = (position + 1) % (NV * NW), (position + NV * NW - 1) % (NV * NW)
    up = {"v": after // NW, "w": after % NW}
    down = {"v": before // NW, "w": before % NW}
    pair = {"v": v + 1 - 2 * member}

    def remote(src, dst, send, recv, device):
        return pltpu.make_async_remote_copy(
            src_ref=src,
            dst_ref=dst,
            send_sem=send,
            recv_sem=recv,
            device_id=device,
            device_id_type=pl.DeviceIdType.MESH,
        )

    def wait_for(ref, sem):
        pltpu.make_async_copy(ref, ref, sem).wait()

    own_half_rows = pl.ds(pl.multiple_of(member * half, half), half)
    other_half_rows = pl.ds(pl.multiple_of((1 - member) * half, half), half)
    key_copy = pltpu.make_async_copy(key_hbm, keys.at[own_half_rows], local_sem.at[0])
    key_copy.start()
    weight_copy = pltpu.make_async_copy(weight_hbm, weight, local_sem.at[1])
    weight_copy.start()
    HC = D // 4
    hidden_copies = [
        pltpu.make_async_copy(
            hidden_hbm.at[:, pl.ds(i * HC, HC)], hidden.at[:, pl.ds(i * HC, HC)], hidden_sem.at[i]
        )
        for i in range(4)
    ]
    for copy in hidden_copies:
        copy.start()
    query_copy = pltpu.make_async_copy(query_hbm, query, local_sem.at[2])
    grad_copy = pltpu.make_async_copy(grad_hbm, grad, local_sem.at[3])
    out_copy = pltpu.make_async_copy(out_hbm, attn_out, local_sem.at[4])
    norm_copy = pltpu.make_async_copy(norm_hbm, norm_ref, local_sem.at[6])
    docs_copy = pltpu.make_async_copy(docs_hbm, docs_ref, local_sem.at[7])
    for copy in (norm_copy, docs_copy, query_copy, grad_copy, out_copy):
        copy.start()

    barrier = pltpu.get_barrier_semaphore()

    def greet(device):
        pl.semaphore_signal(
            barrier, inc=1, device_id=device, device_id_type=pl.DeviceIdType.MESH
        )

    greet({"v": (v + 1) % NV})
    greet({"v": (v + NV - 1) % NV})
    greet(up)
    greet(down)

    def greet_plane(i, carry):
        greet(plane(i)[0])
        return carry

    lax.fori_loop(1, NS, greet_plane, 0)

    def greet_line(i, carry):
        greet({"w": (w + i) % NW})
        return carry

    lax.fori_loop(1, NW, greet_line, 0)

    weight_copy.wait()
    CK = 1024
    total = jnp.zeros((half, T), F32)
    for i in range(4):
        hidden_copies[i].wait()

        def add_values(k, acc, base=i * HC):
            at = pl.ds(pl.multiple_of(base + k * CK, CK), CK)
            return acc + dot(weight[:, at], hidden[:, at], 1, 1)

        total = lax.fori_loop(0, HC // CK, add_values, total)
    values[own_half_rows, :] = total.astype(BF16)
    norm_copy.wait()
    docs_copy.wait()
    norm = jnp.concatenate([norm_ref[...]] * (T // heads), axis=0).T
    rows = lax.broadcasted_iota(jnp.int32, (T, T), 0)
    columns = lax.broadcasted_iota(jnp.int32, (T, T), 1)
    documents = jnp.broadcast_to(docs_ref[...].astype(F32), (T, T))
    allowed = (columns <= rows) & (documents == documents.T)
    key_copy.wait()

    pl.semaphore_wait(barrier, 4 + (NS - 1) + (NW - 1))

    key_exchange = remote(keys.at[own_half_rows], key_recv, pair_send.at[0], pair_recv.at[0], pair)
    key_exchange.start()
    own_rows = pl.ds(pl.multiple_of(row_group * R, R), R)

    def weight_piece(to):
        start = ((to * NY + y) * NC + c) * DS + depth_half * DB
        return weight.at[own_rows, pl.ds(pl.multiple_of(start, DB), DB)]

    for i in range(1, NX):
        to = (x + i) % NX
        remote(
            weight_piece(to),
            plane_weights.at[w, v, x],
            x_sems.at[0],
            x_sems.at[1],
            {"x": to},
        ).start()
    own_copy = pltpu.make_async_copy(
        weight_piece(x), plane_weights.at[w, v, x], local_sem.at[5]
    )
    own_copy.start()
    value_exchange = remote(values.at[own_half_rows], val_recv, pair_send.at[1], pair_recv.at[1], pair)

    own_copy.wait()
    wait_for(plane_weights.at[w, v, pl.ds(0, NX - 1)], x_sems.at[1])

    def weights_to(j):
        block = plane_weights.at[w, v]
        return remote(block, block, v_send.at[j], v_recv.at[j], {"v": (v + j) % NV})

    def weights_on(j):
        first = 0 if j == 1 else NX // 2
        block = plane_weights.at[w, (v + NV - j) % NV, pl.ds(first, NX // 2)]
        return remote(block, block, v_send.at[j - 1], v_recv.at[j - 1], {"v": (v + j) % NV})

    weights_to(1).start()
    weights_to(3).start()

    query_copy.wait()
    grad_copy.wait()
    key_exchange.wait_recv()
    keys[other_half_rows, :] = key_recv[...]

    value_part = jnp.zeros((width, T), F32)
    for h in range(heads):
        lanes = pl.ds(h * width, width)
        scores = dot(query[:, lanes], keys[...], 1, 0) * scale
        prob = jnp.where(allowed, jnp.exp(scores - norm[:, h : h + 1]), 0.0)
        probs[h] = prob
        value_part = value_part + dot(grad[:, lanes], prob.astype(BF16), 0, 0)

    own_half = jnp.where(lower, value_part[:half], value_part[half:])
    half_send[...] = jnp.where(lower, value_part[half:], value_part[:half]).astype(BF16)
    half_exchange = remote(half_send, half_recv, pair_send.at[2], pair_recv.at[2], pair)
    half_exchange.start()
    by_token = value_part.T.reshape(NX, NV, TR, width)
    for i in range(NV):
        part_send[i] = by_token[:, i].reshape(TV, width).astype(BF16)

    def part_to(j):
        to = (v + j) % NV
        return remote(
            part_send.at[to], part_recv.at[v], part_ssem.at[j], part_rsem.at[j], {"v": to}
        )

    for j in (2, 1, 3):
        part_to(j).start()
    part_recv[v] = part_send[v]
    value_exchange.start()

    weights_to(1).wait_recv()
    weights_on(1).start()
    weights_to(3).wait_recv()
    weights_on(3).start()

    half_exchange.wait_recv()
    value_grad_t = (own_half + half_recv[...].astype(F32)).astype(BF16)

    def core_copy(off):
        return remote(
            core_send.at[off],
            core_recv.at[off],
            core_ssem.at[off],
            core_rsem.at[off],
            {"c": 1 - c},
        )

    def make_blocks(off, carry):
        to_w = (w + off) % NW
        for j in range(NY):
            block = (((y + j) % NY) * NW + to_w) * NC
            own = pl.multiple_of((block + c) * BD, BD)
            other = pl.multiple_of((block + 1 - c) * BD, BD)
            core_send[off, j] = dot(value_grad_t, hidden[:, pl.ds(other, BD)], 1, 0).astype(BF16)
            keep[off, j] = dot(value_grad_t, hidden[:, pl.ds(own, BD)], 1, 0)
        core_copy(off).start()
        return carry

    lax.fori_loop(0, NW, make_blocks, 0)

    def send_y(off, carry):
        core_copy(off).wait_recv()
        for j in range(1, NY):
            y_send[off, j - 1] = (keep[off, j] + core_recv[off, j].astype(F32)).astype(BF16)
            remote(
                y_send.at[off, j - 1],
                y_recv.at[off, j - 1],
                y_ssem,
                y_rsem.at[off],
                {"y": (y + j) % NY},
            ).start()
        keep[off, 0] = keep[off, 0] + core_recv[off, 0].astype(F32)
        return carry

    lax.fori_loop(0, NW // 2, send_y, 0)

    weights_on(1).wait_recv()
    weights_on(3).wait_recv()
    UP, DOWN = NW // 2, (NW - 1) // 2
    HV = NV // 2

    def chain_up(k, part):
        block = plane_weights.at[(w + NW - k) % NW, pl.ds(part * HV, HV)]
        return remote(block, block, chain_send.at[0, k, part], chain_recv.at[0, k, part], up)

    def chain_down(k, part):
        block = plane_weights.at[(w + k) % NW, pl.ds(part * HV, HV)]
        return remote(block, block, chain_send.at[1, k, part], chain_recv.at[1, k, part], down)

    for part in range(2):
        chain_up(0, part).start()
        if DOWN:
            chain_down(0, part).start()

    def pass_on(k):
        for part in range(2):
            chain_up(k, part).wait_recv()
            if k + 1 < UP:
                chain_up(k + 1, part).start()
            if k < DOWN:
                chain_down(k, part).wait_recv()
                if k + 1 < DOWN:
                    chain_down(k + 1, part).start()

    for j in (1, 3, 2):
        part_to(j).wait_recv()
    own_tokens = jnp.concatenate(
        [
            part_recv[2 * i].astype(F32) + part_recv[2 * i + 1].astype(F32)
            for i in range(NV // 2)
        ],
        axis=1,
    )
    plane_grads[me] = own_tokens.astype(BF16)

    def send_grads(i, carry):
        remote(
            plane_grads.at[me], plane_grads.at[me], plane_sems.at[0], plane_sems.at[1], plane(i)[0]
        ).start()
        return carry

    lax.fori_loop(1, NS, send_grads, 0)
    lax.fori_loop(NW // 2, NW, send_y, 0)
    pass_on(0)

    out_copy.wait()
    value_exchange.wait_recv()
    values[other_half_rows, :] = val_recv[...]
    key_part = jnp.zeros((width, T), F32)
    for h in range(heads):
        lanes = pl.ds(h * width, width)
        head_grad = grad[:, lanes]
        row_dots = jnp.sum(
            head_grad.astype(F32) * attn_out[:, lanes].astype(F32), axis=1, keepdims=True
        )
        prob_grad = dot(head_grad, values[...], 1, 0)
        score_grad = (probs[h] * (prob_grad - row_dots) * scale).astype(BF16)
        qgrad_ref[:, lanes] = dot(score_grad, keys[...], 1, 1).astype(BF16)
        key_part = key_part + dot(query[:, lanes], score_grad, 0, 0)
    own_kpart = jnp.where(lower, key_part[:half], key_part[half:])
    kpart_send[...] = jnp.where(lower, key_part[half:], key_part[:half]).astype(BF16)
    kpart_exchange = remote(kpart_send, kpart_recv, pair_send.at[3], pair_recv.at[3], pair)
    kpart_exchange.start()
    if UP > 1:
        pass_on(1)

    def send_w(off):
        wait_for(y_recv.at[off], y_rsem.at[off])
        summed = keep[off, 0]
        for j in range(NY - 1):
            summed = summed + y_recv[off, j].astype(F32)
        if off == 0:
            keep[0, 0] = summed
            return
        w_send[off - 1] = summed.astype(BF16)
        remote(
            w_send.at[off - 1],
            w_recv.at[off - 1],
            w_sems.at[0],
            w_sems.at[1],
            {"w": (w + off) % NW},
        ).start()

    pending = list(range(1, NW)) + [0]
    share = -(-NW // UP)
    for k in range(UP):
        for off in pending[k * share : (k + 1) * share]:
            send_w(off)
        if k > 1:
            pass_on(k)

    wait_for(plane_grads.at[pl.ds(0, NS - 1)], plane_sems.at[1])
    NG = NY * NC
    pieces = []
    for d in range(2):
        acc = jnp.zeros((NG * TV, DB), F32)
        for i in range(NX):
            left = plane_grads[i * NG : (i + 1) * NG].reshape(NG * TV, NV * half)
            right = jnp.concatenate(
                [plane_weights[d * RG + g, k, i] for k in range(NV) for g in range(RG)], axis=0
            )
            acc = acc + dot(left, right, 1, 0)
        pieces.append(acc.reshape(NG, NX, TR, DB))
    for i in range(NX):
        out_send[i * NG : (i + 1) * NG] = jnp.concatenate(
            [pieces[0][:, i], pieces[1][:, i]], axis=1
        ).astype(BF16)

    def send_out(i, carry):
        device, slot = plane(i)
        remote(
            out_send.at[slot], out_recv.at[me], plane_sems.at[2], plane_sems.at[3], device
        ).start()
        return carry

    lax.fori_loop(1, NS, send_out, 0)
    out_recv[me] = out_send[me]

    kpart_exchange.wait_recv()
    kgrad_ref[...] = (own_kpart + kpart_recv[...].astype(F32)).astype(BF16)
    wait_for(w_recv, w_sems.at[1])
    summed = keep[0, 0]
    for off in range(NW - 1):
        summed = summed + w_recv[off].astype(F32)
    wgrad_ref[...] = summed
    wait_for(out_recv.at[pl.ds(0, NS - 1)], plane_sems.at[3])
    igrad_ref[...] = out_recv[...]

    for exchange in (key_exchange, value_exchange, half_exchange, kpart_exchange):
        exchange.wait_send()
    wait_for(plane_weights.at[w, v, pl.ds(0, NX - 1)], x_sems.at[0])
    for j in (1, 3):
        weights_to(j).wait_send()
        weights_on(j).wait_send()
    for j in (1, 2, 3):
        part_to(j).wait_send()
    for part in range(2):
        for k in range(UP):
            chain_up(k, part).wait_send()
        for k in range(DOWN):
            chain_down(k, part).wait_send()

    def core_sent(off, carry):
        core_copy(off).wait_send()
        return carry

    lax.fori_loop(0, NW, core_sent, 0)
    wait_for(y_send, y_ssem)
    wait_for(w_send, w_sems.at[0])
    wait_for(plane_grads.at[pl.ds(0, NS - 1)], plane_sems.at[0])
    wait_for(out_send.at[pl.ds(0, NS - 1)], plane_sems.at[2])


def hand_over(*refs):
    sems = refs[-1]
    copies = [
        pltpu.make_async_copy(source, target, sems.at[i])
        for i, (source, target) in enumerate(zip(refs[:4], refs[4:8]))
    ]
    for copy in copies:
        copy.start()
    for copy in copies:
        copy.wait()


def per_device(
    sizes,
    hidden_in,
    value_weight,
    queries,
    key_rows,
    attention_out,
    output_grad,
    log_normalizer,
    document_ids,
):
    NX, NY, NW, NC, NV = sizes
    T, D = hidden_in.shape[1:]
    half = key_rows.shape[2]
    width = 2 * half
    heads = log_normalizer.shape[2]
    NS = NX * NY * NC
    DS = D // NS
    DB = DS // 2
    R = half // (NW // 2)
    TR = T // (NX * NV)
    TV = T // NV
    BD = D // (NY * NW * NC)
    half_block = pltpu.VMEM((half, T), BF16)
    dma = pltpu.SemaphoreType.DMA
    scratch = [
        pltpu.VMEM((heads, T), F32),
        pltpu.VMEM((1, T), jnp.int32),
        pltpu.VMEM((T, D), BF16),
        pltpu.VMEM((half, D), BF16),
        pltpu.VMEM((T, heads * width), BF16),
        pltpu.VMEM((T, heads * width), BF16),
        pltpu.VMEM((T, heads * width), BF16),
        half_block,
        half_block,
        pltpu.VMEM((width, T), BF16),
        pltpu.VMEM((width, T), BF16),
        pltpu.VMEM((heads, T, T), F32),
        half_block,
        half_block,
        half_block,
        half_block,
        pltpu.VMEM((NV, TV, width), BF16),
        pltpu.VMEM((NV, TV, width), BF16),
        pltpu.VMEM((NS, TV, NV * half), BF16),
        pltpu.VMEM((NW, NV, NX, R, DB), BF16),
        pltpu.VMEM((NS, 2 * TR, DB), BF16),
        pltpu.VMEM((NS, 2 * TR, DB), BF16),
        pltpu.VMEM((NW, NY, half, BD), F32),
        pltpu.VMEM((NW, NY, half, BD), BF16),
        pltpu.VMEM((NW, NY, half, BD), BF16),
        pltpu.VMEM((NW, NY - 1, half, BD), BF16),
        pltpu.VMEM((NW, NY - 1, half, BD), BF16),
        pltpu.VMEM((NW - 1, half, BD), BF16),
        pltpu.VMEM((NW - 1, half, BD), BF16),
        dma((8,)),
        dma((4,)),
        dma((4,)),
        dma((4,)),
        dma((2,)),
        dma((NV,)),
        dma((NV,)),
        dma((NV,)),
        dma((NV,)),
        dma((2, NW, 2)),
        dma((2, NW, 2)),
        dma((4,)),
        dma((NW,)),
        dma((NW,)),
        dma,
        dma((NW,)),
        dma((2,)),
    ]
    anywhere = pl.BlockSpec(memory_space=pltpu.HBM)
    vmem = pl.BlockSpec(memory_space=pltpu.VMEM)
    results = pl.pallas_call(
        functools.partial(kernel, sizes),
        out_shape=(
            jax.ShapeDtypeStruct((T, heads * width), BF16),
            jax.ShapeDtypeStruct((half, T), BF16),
            jax.ShapeDtypeStruct((NS, 2 * TR, DB), BF16),
            jax.ShapeDtypeStruct((half, BD), F32),
        ),
        in_specs=[anywhere] * 8,
        out_specs=(vmem,) * 4,
        scratch_shapes=scratch,
        compiler_params=pltpu.CompilerParams(
            collective_id=0, has_side_effects=True, vmem_limit_bytes=48 * 1024 * 1024
        ),
    )(
        *(
            pltpu.with_memory_space_constraint(array, pltpu.HBM)
            for array in (
                hidden_in[0],
                value_weight.T,
                queries[0],
                key_rows[0].T,
                attention_out[0],
                output_grad[0],
                log_normalizer[0].T,
                document_ids,
            )
        )
    )
    query_grad, key_grad, input_blocks, weight_grad = pl.pallas_call(
        hand_over,
        out_shape=tuple(jax.ShapeDtypeStruct(r.shape, r.dtype) for r in results),
        in_specs=(vmem,) * 4,
        out_specs=(anywhere,) * 4,
        scratch_shapes=[dma((4,))],
        compiler_params=pltpu.CompilerParams(vmem_limit_bytes=8 * 1024 * 1024),
    )(*results)
    input_grad = (
        input_blocks.reshape(NS, 2, TR, DB).transpose(2, 0, 1, 3).reshape(1, TR, D)
    )
    return query_grad[None], key_grad.T[None], input_grad, weight_grad.T


def over(finer):
    sizes = tuple(finer.shape[name] for name in ("x", "y", "w", "c", "v"))
    return jax.shard_map(
        functools.partial(per_device, sizes),
        mesh=finer,
        in_specs=(
            P(DP, None, None),
            P(None, TENSOR),
            P(DP, None, TENSOR),
            P(DP, None, TENSOR),
            P(DP, None, TENSOR),
            P(DP, None, TENSOR),
            P(DP, None, TENSOR),
            P(DP, None),
        ),
        out_specs=(P(DP, None, TENSOR), P(DP, None, TENSOR), P(DP, TENSOR, None), P(DP, TENSOR)),
        check_vma=False,
    )


def solution(mesh):
    return over(Mesh(mesh.devices.reshape(4, 8, 2, 4, 4), DP + TENSOR))
```

```python
import functools
import math

import jax
import jax.numpy as jnp
from jax import lax
from jax.experimental import pallas as pl
from jax.experimental.pallas import tpu as pltpu
from jax.sharding import Mesh
from jax.sharding import PartitionSpec as P

DP = ("y", "w", "c")
TENSOR = ("x", "v")
BF16 = jnp.bfloat16
F32 = jnp.float32


def dot(a, b, da, db):
    return lax.dot_general(a, b, (((da,), (db,)), ((), ())), preferred_element_type=F32)


def kernel(
    sizes,
    hidden_hbm,
    weight_hbm,
    query_hbm,
    key_hbm,
    out_hbm,
    grad_hbm,
    norm_hbm,
    docs_hbm,
    qgrad_ref,
    kgrad_ref,
    igrad_ref,
    wgrad_ref,
    norm_ref,
    docs_ref,
    hidden,
    weight,
    weight_send,
    query,
    attn_out,
    grad,
    key_recv,
    val_recv,
    keys,
    values,
    probs,
    half_send,
    half_recv,
    kpart_send,
    kpart_recv,
    part_send,
    part_recv,
    plane_grads,
    plane_weights,
    out_send,
    out_recv,
    keep,
    core_send,
    core_recv,
    far_send,
    far_recv,
    y_send,
    y_recv,
    w_send,
    w_recv,
    local_sem,
    hidden_sem,
    piece_sem,
    pair_send,
    pair_recv,
    x_sems,
    v_send,
    v_recv,
    part_ssem,
    part_rsem,
    chain_send,
    chain_recv,
    plane_sems,
    core_ssem,
    core_rsem,
    far_ssem,
    far_rsem,
    y_ssem,
    y_rsem,
    w_ssem,
    w_rsem,
):
    NX, NY, NW, NC, NV = sizes
    T, D = hidden.shape
    half = weight.shape[0]
    width = 2 * half
    heads = norm_ref.shape[0]
    scale = 1.0 / math.sqrt(width)
    NS = NX * NY * NC
    DS = D // NS
    DB = DS // 2
    RG = NW // 2
    R = half // RG
    TR = T // (NX * NV)
    TV = T // NV
    BD = D // (NY * NW * NC)
    x, y, w, c, v = (lax.axis_index(name) for name in ("x", "y", "w", "c", "v"))
    me = (x * NY + y) * NC + c
    member = v % 2
    lower = member == 0
    depth_half, row_group = w // RG, w % RG

    def plane(i):
        dx, dy, dc = i // (NY * NC), (i // NC) % NY, i % NC
        px, py, pc = (x + dx) % NX, (y + dy) % NY, (c + dc) % NC
        return {"x": px, "y": py, "c": pc}, (px * NY + py) * NC + pc

    position = v * NW + w
    after, before = (position + 1) % (NV * NW), (position + NV * NW - 1) % (NV * NW)
    up = {"v": after // NW, "w": after % NW}
    down = {"v": before // NW, "w": before % NW}
    pair = {"v": v + 1 - 2 * member}

    def remote(src, dst, send, recv, device):
        return pltpu.make_async_remote_copy(
            src_ref=src,
            dst_ref=dst,
            send_sem=send,
            recv_sem=recv,
            device_id=device,
            device_id_type=pl.DeviceIdType.MESH,
        )

    def wait_for(ref, sem):
        pltpu.make_async_copy(ref, ref, sem).wait()

    barrier = pltpu.get_barrier_semaphore()

    def greet(device):
        pl.semaphore_signal(
            barrier, inc=1, device_id=device, device_id_type=pl.DeviceIdType.MESH
        )

    greet({"v": (v + 1) % NV})
    greet({"v": (v + NV - 1) % NV})

    own_half_rows = pl.ds(pl.multiple_of(member * half, half), half)
    other_half_rows = pl.ds(pl.multiple_of((1 - member) * half, half), half)
    key_copy = pltpu.make_async_copy(key_hbm, keys.at[own_half_rows], local_sem.at[0])
    key_copy.start()
    own_rows = pl.ds(pl.multiple_of(row_group * R, R), R)
    piece_copies = []
    for i in range(NX):
        to = (x + i) % NX
        start = ((to * NY + y) * NC + c) * DS + depth_half * DB
        piece_copies.append(
            pltpu.make_async_copy(
                weight_hbm.at[own_rows, pl.ds(pl.multiple_of(start, DB), DB)],
                weight_send.at[i] if i else plane_weights.at[w, v, x],
                piece_sem.at[i],
            )
        )
        piece_copies[i].start()
    norm_copy = pltpu.make_async_copy(norm_hbm, norm_ref, local_sem.at[5])
    docs_copy = pltpu.make_async_copy(docs_hbm, docs_ref, local_sem.at[6])
    weight_copy = pltpu.make_async_copy(weight_hbm, weight, local_sem.at[1])
    for copy in (norm_copy, docs_copy, weight_copy):
        copy.start()
    HC = D // 4
    hidden_copies = [
        pltpu.make_async_copy(
            hidden_hbm.at[:, pl.ds(i * HC, HC)], hidden.at[:, pl.ds(i * HC, HC)], hidden_sem.at[i]
        )
        for i in range(4)
    ]
    query_copy = pltpu.make_async_copy(query_hbm, query, local_sem.at[2])
    grad_copy = pltpu.make_async_copy(grad_hbm, grad, local_sem.at[3])
    out_copy = pltpu.make_async_copy(out_hbm, attn_out, local_sem.at[4])
    for copy in (*hidden_copies, query_copy, grad_copy, out_copy):
        copy.start()

    greet(up)
    greet(down)

    def greet_plane(i, carry):
        greet(plane(i)[0])
        return carry

    lax.fori_loop(1, NS, greet_plane, 0)

    def greet_line(i, carry):
        greet({"w": (w + i) % NW})
        return carry

    lax.fori_loop(1, NW, greet_line, 0)

    key_copy.wait()
    for copy in piece_copies:
        copy.wait()
    pl.semaphore_wait(barrier, 4 + (NS - 1) + (NW - 1))

    key_exchange = remote(keys.at[own_half_rows], key_recv, pair_send.at[0], pair_recv.at[0], pair)
    key_exchange.start()
    for i in range(1, NX):
        remote(
            weight_send.at[i],
            plane_weights.at[w, v, x],
            x_sems.at[0],
            x_sems.at[1],
            {"x": (x + i) % NX},
        ).start()

    weight_copy.wait()

    norm_copy.wait()
    docs_copy.wait()
    norm = jnp.concatenate([norm_ref[...]] * (T // heads), axis=0).T
    rows = lax.broadcasted_iota(jnp.int32, (T, T), 0)
    columns = lax.broadcasted_iota(jnp.int32, (T, T), 1)
    documents = jnp.broadcast_to(docs_ref[...].astype(F32), (T, T))
    allowed = (columns <= rows) & (documents == documents.T)
    CK = 1024

    def add_values(k, acc):
        at = pl.ds(pl.multiple_of(k * CK, CK), CK)
        return acc + dot(weight[:, at], hidden[:, at], 1, 1)

    total = jnp.zeros((half, T), F32)
    for i in range(2):
        hidden_copies[i].wait()
        total = lax.fori_loop(i * HC // CK, (i + 1) * HC // CK, add_values, total)

    wait_for(plane_weights.at[w, v, pl.ds(0, NX - 1)], x_sems.at[1])

    def weights_to(j):
        block = plane_weights.at[w, v]
        return remote(block, block, v_send.at[j], v_recv.at[j], {"v": (v + j) % NV})

    def weights_on(j):
        first = 0 if j == 1 else NX // 2
        block = plane_weights.at[w, (v + NV - j) % NV, pl.ds(first, NX // 2)]
        return remote(block, block, v_send.at[j - 1], v_recv.at[j - 1], {"v": (v + j) % NV})

    weights_to(1).start()
    weights_to(3).start()

    for i in range(2, 4):
        hidden_copies[i].wait()
        total = lax.fori_loop(i * HC // CK, (i + 1) * HC // CK, add_values, total)
    values[own_half_rows, :] = total.astype(BF16)

    query_copy.wait()
    grad_copy.wait()
    key_exchange.wait_recv()
    keys[other_half_rows, :] = key_recv[...]

    value_part = jnp.zeros((width, T), F32)
    for h in range(heads):
        lanes = pl.ds(h * width, width)
        scores = dot(query[:, lanes], keys[...], 1, 0) * scale
        prob = jnp.where(allowed, jnp.exp(scores - norm[:, h : h + 1]), 0.0)
        probs[h] = prob
        value_part = value_part + dot(grad[:, lanes], prob.astype(BF16), 0, 0)

    own_half = jnp.where(lower, value_part[:half], value_part[half:])
    half_send[...] = jnp.where(lower, value_part[half:], value_part[:half]).astype(BF16)
    half_exchange = remote(half_send, half_recv, pair_send.at[2], pair_recv.at[2], pair)
    half_exchange.start()
    by_token = value_part.T.reshape(NX, NV, TR, width)
    for i in range(NV):
        part_send[i] = by_token[:, i].reshape(TV, width).astype(BF16)

    def part_to(j):
        to = (v + j) % NV
        return remote(
            part_send.at[to], part_recv.at[v], part_ssem.at[j], part_rsem.at[j], {"v": to}
        )

    for j in (2, 1, 3):
        part_to(j).start()
    part_recv[v] = part_send[v]
    def spread(i, carry):
        residue = (w + i) % NW
        at = pl.ds(pl.multiple_of(residue % RG * R, R), R)
        for k in range(NX):
            to = (x + k) % NX
            start = ((to * NY + y) * NC + c) * DS + residue // RG * DB
            source = weight.at[at, pl.ds(pl.multiple_of(start, DB), DB)]
            target = plane_weights.at[residue, v, x]
            if k:
                remote(source, target, x_sems.at[2], x_sems.at[3], {"x": to}).start()
            else:
                pltpu.make_async_copy(source, target, local_sem.at[7]).start()
        return carry

    lax.fori_loop(1, NW, spread, 0)

    weights_to(1).wait_recv()
    weights_on(1).start()
    weights_to(3).wait_recv()
    weights_on(3).start()

    UP, DOWN = NW // 2, (NW - 1) // 2
    PIECES = ((3, 2, 1), (1, 2, 3))

    def chain(way, k, q):
        origin = (position + (NV * NW - k if way == 0 else k)) % (NV * NW)
        to = (up, down)[way]
        block = plane_weights.at[origin % NW, (to["v"] + q) % NV]
        return remote(block, block, chain_send.at[way, k, q], chain_recv.at[way, k, q], to)

    def start_chain():
        for qs in zip(*PIECES):
            for way, steps in enumerate((UP, DOWN)):
                if steps:
                    chain(way, 0, qs[way]).start()

    def pass_on(k):
        for qs in zip(*PIECES):
            for way, steps in enumerate((UP, DOWN)):
                if k < steps:
                    chain(way, k, qs[way]).wait_recv()
                if k + 1 < steps:
                    chain(way, k + 1, qs[way]).start()

    value_exchange = remote(values.at[own_half_rows], val_recv, pair_send.at[1], pair_recv.at[1], pair)
    value_exchange.start()

    half_exchange.wait_recv()
    value_grad_t = (own_half + half_recv[...].astype(F32)).astype(BF16)

    def core_copy(off):
        return remote(
            core_send.at[off],
            core_recv.at[off],
            core_ssem.at[off],
            core_rsem.at[off],
            {"c": 1 - c},
        )

    def make_blocks(off, carry):
        to_w = (w + off) % NW
        for j in range(NY):
            block = (((y + j) % NY) * NW + to_w) * NC
            own = pl.multiple_of((block + c) * BD, BD)
            other = pl.multiple_of((block + 1 - c) * BD, BD)
            core_send[off, j] = dot(value_grad_t, hidden[:, pl.ds(other, BD)], 1, 0).astype(BF16)
            keep[off, j] = dot(value_grad_t, hidden[:, pl.ds(own, BD)], 1, 0)
        core_copy(off).start()
        return carry

    lax.fori_loop(0, NW, make_blocks, 0)

    quarter = half // 2

    def part_sum(off, j):
        return keep[off, j] + core_recv[off, j].astype(F32)

    def far_copy(off, way):
        at = pl.ds(way * quarter, quarter)
        return remote(
            far_send.at[off, at],
            far_recv.at[off, at],
            far_ssem,
            far_rsem.at[off],
            {"y": (y + (1, NY - 1)[way]) % NY},
        )

    def y_copy(off, way):
        return remote(
            y_send.at[off, way],
            y_recv.at[off, way],
            y_ssem,
            y_rsem.at[off],
            {"y": (y + (1, NY - 1)[way]) % NY},
        )

    def send_far(off, carry):
        core_copy(off).wait_recv()
        far_send[off] = part_sum(off, 2).astype(BF16)
        far_copy(off, 0).start()
        far_copy(off, 1).start()
        return carry

    def send_y(off, carry):
        wait_for(far_recv.at[off], far_rsem.at[off])
        came = far_recv[off].astype(F32)
        right, left = part_sum(off, 1), part_sum(off, 3)
        y_send[off, 0] = jnp.concatenate(
            [right[:quarter] + came[:quarter], right[quarter:]], axis=0
        ).astype(BF16)
        y_copy(off, 0).start()
        y_send[off, 1] = jnp.concatenate(
            [left[:quarter], left[quarter:] + came[quarter:]], axis=0
        ).astype(BF16)
        y_copy(off, 1).start()
        return carry

    lax.fori_loop(0, NW, send_far, 0)
    weights_on(1).wait_recv()
    weights_on(3).wait_recv()
    spread_blocks = plane_weights.at[pl.ds(0, NW - 1), 0, pl.ds(0, NX - 1)]
    wait_for(spread_blocks, x_sems.at[3])
    wait_for(plane_weights.at[pl.ds(0, NW - 1), 0, 0], local_sem.at[7])
    start_chain()

    lax.fori_loop(0, NW, send_y, 0)

    out_copy.wait()
    value_exchange.wait_recv()
    values[other_half_rows, :] = val_recv[...]
    key_part = jnp.zeros((width, T), F32)
    for h in range(heads):
        lanes = pl.ds(h * width, width)
        head_grad = grad[:, lanes]
        row_dots = jnp.sum(
            head_grad.astype(F32) * attn_out[:, lanes].astype(F32), axis=1, keepdims=True
        )
        prob_grad = dot(head_grad, values[...], 1, 0)
        score_grad = (probs[h] * (prob_grad - row_dots) * scale).astype(BF16)
        qgrad_ref[:, lanes] = dot(score_grad, keys[...], 1, 1).astype(BF16)
        key_part = key_part + dot(query[:, lanes], score_grad, 0, 0)
    own_kpart = jnp.where(lower, key_part[:half], key_part[half:])
    kpart_send[...] = jnp.where(lower, key_part[half:], key_part[:half]).astype(BF16)
    kpart_exchange = remote(kpart_send, kpart_recv, pair_send.at[3], pair_recv.at[3], pair)
    kpart_exchange.start()

    pass_on(0)

    for j in (1, 3, 2):
        part_to(j).wait_recv()
    own_tokens = jnp.concatenate(
        [
            part_recv[2 * i].astype(F32) + part_recv[2 * i + 1].astype(F32)
            for i in range(NV // 2)
        ],
        axis=1,
    )
    chips = NX * NY
    plane_grads[c, x * NY + y] = own_tokens.astype(BF16)

    def send_grads(i, carry):
        px, py = (x + i // NY) % NX, (y + i % NY) % NY
        block = plane_grads.at[c, x * NY + y]
        remote(block, block, plane_sems.at[0], plane_sems.at[1], {"x": px, "y": py}).start()
        return carry

    lax.fori_loop(1, chips, send_grads, 0)
    grads_over = remote(
        plane_grads.at[c], plane_grads.at[c], plane_sems.at[4], plane_sems.at[5], {"c": 1 - c}
    )

    def share_grads():
        wait_for(plane_grads.at[c, pl.ds(0, chips - 1)], plane_sems.at[1])
        grads_over.start()


    def send_w(off):
        wait_for(y_recv.at[off], y_rsem.at[off])
        summed = part_sum(off, 0) + y_recv[off, 0].astype(F32) + y_recv[off, 1].astype(F32)
        if off == 0:
            keep[0, 0] = summed
            return
        w_send[off - 1] = summed.astype(BF16)
        remote(
            w_send.at[off - 1],
            w_recv.at[off - 1],
            w_ssem,
            w_rsem,
            {"w": (w + off) % NW},
        ).start()

    pending = list(range(1, NW)) + [0]
    for off in pending[: NW // 2]:
        send_w(off)
    pass_on(1)
    for off in pending[NW // 2 :]:
        send_w(off)

    share_grads()
    for k in range(2, UP):
        pass_on(k)

    grads_over.wait_recv()
    NG = NY * NC
    pieces = []
    for d in range(2):
        acc = jnp.zeros((NG * TV, DB), F32)
        for i in range(NX):
            left = jnp.concatenate(
                [
                    plane_grads[k, i * NY : (i + 1) * NY].reshape(NY * TV, NV * half)
                    for k in range(NC)
                ],
                axis=0,
            )
            right = jnp.concatenate(
                [plane_weights[d * RG + g, k, i] for k in range(NV) for g in range(RG)], axis=0
            )
            acc = acc + dot(left, right, 1, 0)
        pieces.append(acc.reshape(NC, NY, NX, TR, DB))
    for i in range(NX):
        for j in range(NY):
            for k in range(NC):
                out_send[(i * NY + j) * NC + k] = jnp.concatenate(
                    [pieces[0][k, j, i], pieces[1][k, j, i]], axis=0
                ).astype(BF16)

    def send_out(i, carry):
        device, slot = plane(i)
        remote(
            out_send.at[slot], out_recv.at[me], plane_sems.at[2], plane_sems.at[3], device
        ).start()
        return carry

    lax.fori_loop(1, NS, send_out, 0)
    out_recv[me] = out_send[me]

    kpart_exchange.wait_recv()
    kgrad_ref[...] = (own_kpart + kpart_recv[...].astype(F32)).astype(BF16)
    wait_for(w_recv, w_rsem)
    summed = keep[0, 0]
    for off in range(NW - 1):
        summed = summed + w_recv[off].astype(F32)
    wgrad_ref[...] = summed
    wait_for(out_recv.at[pl.ds(0, NS - 1)], plane_sems.at[3])
    igrad_ref[...] = out_recv[...]

    for exchange in (key_exchange, value_exchange, half_exchange, kpart_exchange):
        exchange.wait_send()
    wait_for(plane_weights.at[w, v, pl.ds(0, NX - 1)], x_sems.at[0])
    for j in (1, 3):
        weights_to(j).wait_send()
        weights_on(j).wait_send()
    for j in (1, 2, 3):
        part_to(j).wait_send()
    wait_for(spread_blocks, x_sems.at[2])
    for way, steps in enumerate((UP, DOWN)):
        for k in range(steps):
            for q in PIECES[way]:
                chain(way, k, q).wait_send()

    def core_sent(off, carry):
        core_copy(off).wait_send()
        return carry

    lax.fori_loop(0, NW, core_sent, 0)
    wait_for(far_send, far_ssem)
    wait_for(y_send, y_ssem)
    wait_for(w_send, w_ssem)
    wait_for(plane_grads.at[c, pl.ds(0, chips - 1)], plane_sems.at[0])
    grads_over.wait_send()
    wait_for(out_send.at[pl.ds(0, NS - 1)], plane_sems.at[2])


def hand_over(*refs):
    sems = refs[-1]
    copies = [
        pltpu.make_async_copy(source, target, sems.at[i])
        for i, (source, target) in enumerate(zip(refs[:4], refs[4:8]))
    ]
    for copy in copies:
        copy.start()
    for copy in copies:
        copy.wait()


def per_device(
    sizes,
    hidden_in,
    value_weight,
    queries,
    key_rows,
    attention_out,
    output_grad,
    log_normalizer,
    document_ids,
):
    NX, NY, NW, NC, NV = sizes
    T, D = hidden_in.shape[1:]
    half = key_rows.shape[2]
    width = 2 * half
    heads = log_normalizer.shape[2]
    NS = NX * NY * NC
    DS = D // NS
    DB = DS // 2
    R = half // (NW // 2)
    TR = T // (NX * NV)
    TV = T // NV
    BD = D // (NY * NW * NC)
    half_block = pltpu.VMEM((half, T), BF16)
    dma = pltpu.SemaphoreType.DMA
    scratch = [
        pltpu.VMEM((heads, T), F32),
        pltpu.VMEM((1, T), jnp.int32),
        pltpu.VMEM((T, D), BF16),
        pltpu.VMEM((half, D), BF16),
        pltpu.VMEM((NX, R, DB), BF16),
        pltpu.VMEM((T, heads * width), BF16),
        pltpu.VMEM((T, heads * width), BF16),
        pltpu.VMEM((T, heads * width), BF16),
        half_block,
        half_block,
        pltpu.VMEM((width, T), BF16),
        pltpu.VMEM((width, T), BF16),
        pltpu.VMEM((heads, T, T), F32),
        half_block,
        half_block,
        half_block,
        half_block,
        pltpu.VMEM((NV, TV, width), BF16),
        pltpu.VMEM((NV, TV, width), BF16),
        pltpu.VMEM((NC, NX * NY, TV, NV * half), BF16),
        pltpu.VMEM((NW, NV, NX, R, DB), BF16),
        pltpu.VMEM((NS, 2 * TR, DB), BF16),
        pltpu.VMEM((NS, 2 * TR, DB), BF16),
        pltpu.VMEM((NW, NY, half, BD), F32),
        pltpu.VMEM((NW, NY, half, BD), BF16),
        pltpu.VMEM((NW, NY, half, BD), BF16),
        pltpu.VMEM((NW, half, BD), BF16),
        pltpu.VMEM((NW, half, BD), BF16),
        pltpu.VMEM((NW, 2, half, BD), BF16),
        pltpu.VMEM((NW, 2, half, BD), BF16),
        pltpu.VMEM((NW - 1, half, BD), BF16),
        pltpu.VMEM((NW - 1, half, BD), BF16),
        dma((8,)),
        dma((4,)),
        dma((NX,)),
        dma((4,)),
        dma((4,)),
        dma((4,)),
        dma((NV,)),
        dma((NV,)),
        dma((NV,)),
        dma((NV,)),
        dma((2, NW // 2, NV)),
        dma((2, NW // 2, NV)),
        dma((6,)),
        dma((NW,)),
        dma((NW,)),
        dma,
        dma((NW,)),
        dma,
        dma((NW,)),
        dma,
        dma,
    ]
    anywhere = pl.BlockSpec(memory_space=pltpu.HBM)
    vmem = pl.BlockSpec(memory_space=pltpu.VMEM)
    results = pl.pallas_call(
        functools.partial(kernel, sizes),
        out_shape=(
            jax.ShapeDtypeStruct((T, heads * width), BF16),
            jax.ShapeDtypeStruct((half, T), BF16),
            jax.ShapeDtypeStruct((NS, 2 * TR, DB), BF16),
            jax.ShapeDtypeStruct((half, BD), F32),
        ),
        in_specs=[anywhere] * 8,
        out_specs=(vmem,) * 4,
        scratch_shapes=scratch,
        compiler_params=pltpu.CompilerParams(
            collective_id=0, has_side_effects=True, vmem_limit_bytes=48 * 1024 * 1024
        ),
    )(
        *(
            pltpu.with_memory_space_constraint(array, pltpu.HBM)
            for array in (
                hidden_in[0],
                value_weight.T,
                queries[0],
                key_rows[0].T,
                attention_out[0],
                output_grad[0],
                log_normalizer[0].T,
                document_ids,
            )
        )
    )
    query_grad, key_grad, input_blocks, weight_grad = pl.pallas_call(
        hand_over,
        out_shape=tuple(jax.ShapeDtypeStruct(r.shape, r.dtype) for r in results),
        in_specs=(vmem,) * 4,
        out_specs=(anywhere,) * 4,
        scratch_shapes=[dma((4,))],
        compiler_params=pltpu.CompilerParams(vmem_limit_bytes=8 * 1024 * 1024),
    )(*results)
    input_grad = (
        input_blocks.reshape(NS, 2, TR, DB).transpose(2, 0, 1, 3).reshape(1, TR, D)
    )
    return query_grad[None], key_grad.T[None], input_grad, weight_grad.T


def over(finer):
    sizes = tuple(finer.shape[name] for name in ("x", "y", "w", "c", "v"))
    return jax.shard_map(
        functools.partial(per_device, sizes),
        mesh=finer,
        in_specs=(
            P(DP, None, None),
            P(None, TENSOR),
            P(DP, None, TENSOR),
            P(DP, None, TENSOR),
            P(DP, None, TENSOR),
            P(DP, None, TENSOR),
            P(DP, None, TENSOR),
            P(DP, None),
        ),
        out_specs=(P(DP, None, TENSOR), P(DP, None, TENSOR), P(DP, TENSOR, None), P(DP, TENSOR)),
        check_vma=False,
    )


def solution(mesh):
    return over(Mesh(mesh.devices.reshape(4, 8, 2, 4, 4), DP + TENSOR))
```

```python
import functools
import math

import jax
import jax.numpy as jnp
from jax import lax
from jax.experimental import pallas as pl
from jax.experimental.pallas import tpu as pltpu
from jax.sharding import Mesh
from jax.sharding import PartitionSpec as P

DP = ("y", "w", "c")
TENSOR = ("x", "v")
BF16 = jnp.bfloat16
F32 = jnp.float32


def dot(a, b, da, db):
    return lax.dot_general(a, b, (((da,), (db,)), ((), ())), preferred_element_type=F32)


def kernel(
    sizes,
    hidden_hbm,
    weight_hbm,
    query_hbm,
    key_hbm,
    out_hbm,
    grad_hbm,
    norm_hbm,
    docs_hbm,
    qgrad_ref,
    kgrad_ref,
    igrad_ref,
    wgrad_ref,
    norm_ref,
    docs_ref,
    hidden,
    weight,
    weight_send,
    query,
    attn_out,
    grad,
    key_recv,
    val_recv,
    keys,
    values,
    probs,
    half_send,
    half_recv,
    kpart_send,
    kpart_recv,
    part_send,
    part_recv,
    plane_grads,
    plane_weights,
    out_send,
    out_recv,
    keep,
    core_send,
    core_recv,
    far_send,
    far_recv,
    y_send,
    y_recv,
    w_send,
    w_recv,
    local_sem,
    hidden_sem,
    piece_sem,
    pair_send,
    pair_recv,
    x_sems,
    v_send,
    v_recv,
    part_ssem,
    part_rsem,
    chain_send,
    chain_recv,
    plane_sems,
    core_ssem,
    core_rsem,
    far_ssem,
    far_rsem,
    y_ssem,
    y_rsem,
    w_ssem,
    w_rsem,
):
    NX, NY, NW, NC, NV = sizes
    T, D = hidden.shape
    half = weight.shape[0]
    width = 2 * half
    heads = norm_ref.shape[0]
    scale = 1.0 / math.sqrt(width)
    NS = NX * NY * NC
    DS = D // NS
    DB = DS // 2
    RG = NW // 2
    R = half // RG
    TR = T // (NX * NV)
    TV = T // NV
    BD = D // (NY * NW * NC)
    x, y, w, c, v = (lax.axis_index(name) for name in ("x", "y", "w", "c", "v"))
    me = (x * NY + y) * NC + c
    member = v % 2
    lower = member == 0
    depth_half, row_group = w // RG, w % RG

    def plane(i):
        dx, dy, dc = i // (NY * NC), (i // NC) % NY, i % NC
        px, py, pc = (x + dx) % NX, (y + dy) % NY, (c + dc) % NC
        return {"x": px, "y": py, "c": pc}, (px * NY + py) * NC + pc

    beside = w + 1 - 2 * (w % 2)
    position = v * NW + w
    after, before = (position + 1) % (NV * NW), (position + NV * NW - 1) % (NV * NW)
    up = {"v": after // NW, "w": after % NW}
    down = {"v": before // NW, "w": before % NW}
    pair = {"v": v + 1 - 2 * member}

    def remote(src, dst, send, recv, device):
        return pltpu.make_async_remote_copy(
            src_ref=src,
            dst_ref=dst,
            send_sem=send,
            recv_sem=recv,
            device_id=device,
            device_id_type=pl.DeviceIdType.MESH,
        )

    def wait_for(ref, sem):
        pltpu.make_async_copy(ref, ref, sem).wait()

    barrier = pltpu.get_barrier_semaphore()

    def greet(device):
        pl.semaphore_signal(
            barrier, inc=1, device_id=device, device_id_type=pl.DeviceIdType.MESH
        )

    greet({"v": (v + 1) % NV})
    greet({"v": (v + NV - 1) % NV})

    own_half_rows = pl.ds(pl.multiple_of(member * half, half), half)
    other_half_rows = pl.ds(pl.multiple_of((1 - member) * half, half), half)
    key_copy = pltpu.make_async_copy(key_hbm, keys.at[own_half_rows], local_sem.at[0])
    key_copy.start()
    own_rows = pl.ds(pl.multiple_of(row_group * R, R), R)
    piece_copies = []
    for i in range(NX):
        to = (x + i) % NX
        start = ((to * NY + y) * NC + c) * DS + depth_half * DB
        piece_copies.append(
            pltpu.make_async_copy(
                weight_hbm.at[own_rows, pl.ds(pl.multiple_of(start, DB), DB)],
                weight_send.at[i] if i else plane_weights.at[w, v, x],
                piece_sem.at[i],
            )
        )
        piece_copies[i].start()
    norm_copy = pltpu.make_async_copy(norm_hbm, norm_ref, local_sem.at[5])
    docs_copy = pltpu.make_async_copy(docs_hbm, docs_ref, local_sem.at[6])
    weight_copy = pltpu.make_async_copy(weight_hbm, weight, local_sem.at[1])
    for copy in (norm_copy, docs_copy, weight_copy):
        copy.start()
    HC = D // 4
    hidden_copies = [
        pltpu.make_async_copy(
            hidden_hbm.at[:, pl.ds(i * HC, HC)], hidden.at[:, pl.ds(i * HC, HC)], hidden_sem.at[i]
        )
        for i in range(4)
    ]
    query_copy = pltpu.make_async_copy(query_hbm, query, local_sem.at[2])
    grad_copy = pltpu.make_async_copy(grad_hbm, grad, local_sem.at[3])
    out_copy = pltpu.make_async_copy(out_hbm, attn_out, local_sem.at[4])
    for copy in (*hidden_copies, query_copy, grad_copy, out_copy):
        copy.start()

    greet(up)
    greet(down)

    def greet_plane(i, carry):
        greet(plane(i)[0])
        return carry

    lax.fori_loop(1, NS, greet_plane, 0)

    for i in range(1, NW // 2):
        greet({"w": (w + 2 * i) % NW})
    greet({"w": beside})

    key_copy.wait()
    for copy in piece_copies:
        copy.wait()
    pl.semaphore_wait(barrier, 4 + (NS - 1) + NW // 2)

    key_exchange = remote(keys.at[own_half_rows], key_recv, pair_send.at[0], pair_recv.at[0], pair)
    key_exchange.start()
    for i in range(1, NX):
        remote(
            weight_send.at[i],
            plane_weights.at[w, v, x],
            x_sems.at[0],
            x_sems.at[1],
            {"x": (x + i) % NX},
        ).start()

    weight_copy.wait()

    norm_copy.wait()
    docs_copy.wait()
    norm = jnp.concatenate([norm_ref[...]] * (T // heads), axis=0).T
    rows = lax.broadcasted_iota(jnp.int32, (T, T), 0)
    columns = lax.broadcasted_iota(jnp.int32, (T, T), 1)
    documents = jnp.broadcast_to(docs_ref[...].astype(F32), (T, T))
    allowed = (columns <= rows) & (documents == documents.T)
    CK = 1024

    def add_values(k, acc):
        at = pl.ds(pl.multiple_of(k * CK, CK), CK)
        return acc + dot(weight[:, at], hidden[:, at], 1, 1)

    total = jnp.zeros((half, T), F32)
    for i in range(2):
        hidden_copies[i].wait()
        total = lax.fori_loop(i * HC // CK, (i + 1) * HC // CK, add_values, total)

    wait_for(plane_weights.at[w, v, pl.ds(0, NX - 1)], x_sems.at[1])

    def weights_to(j):
        block = plane_weights.at[w, v]
        return remote(block, block, v_send.at[j], v_recv.at[j], {"v": (v + j) % NV})

    def weights_on(j):
        first = 0 if j == 1 else NX // 2
        block = plane_weights.at[w, (v + NV - j) % NV, pl.ds(first, NX // 2)]
        return remote(block, block, v_send.at[j - 1], v_recv.at[j - 1], {"v": (v + j) % NV})

    weights_to(1).start()
    weights_to(3).start()

    for i in range(2, 4):
        hidden_copies[i].wait()
        total = lax.fori_loop(i * HC // CK, (i + 1) * HC // CK, add_values, total)
    values[own_half_rows, :] = total.astype(BF16)

    query_copy.wait()
    grad_copy.wait()
    key_exchange.wait_recv()
    keys[other_half_rows, :] = key_recv[...]

    value_part = jnp.zeros((width, T), F32)
    for h in range(heads):
        lanes = pl.ds(h * width, width)
        scores = dot(query[:, lanes], keys[...], 1, 0) * scale
        prob = jnp.where(allowed, jnp.exp(scores - norm[:, h : h + 1]), 0.0)
        probs[h] = prob
        value_part = value_part + dot(grad[:, lanes], prob.astype(BF16), 0, 0)

    own_half = jnp.where(lower, value_part[:half], value_part[half:])
    half_send[...] = jnp.where(lower, value_part[half:], value_part[:half]).astype(BF16)
    half_exchange = remote(half_send, half_recv, pair_send.at[2], pair_recv.at[2], pair)
    half_exchange.start()
    by_token = value_part.T.reshape(NX, NV, TR, width)
    for i in range(NV):
        part_send[i] = by_token[:, i].reshape(TV, width).astype(BF16)

    def part_to(j):
        to = (v + j) % NV
        return remote(
            part_send.at[to], part_recv.at[v], part_ssem.at[j], part_rsem.at[j], {"v": to}
        )

    for j in (2, 1, 3):
        part_to(j).start()
    part_recv[v] = part_send[v]
    def spread(i, carry):
        residue = (w + i) % NW
        at = pl.ds(pl.multiple_of(residue % RG * R, R), R)
        for k in range(NX):
            to = (x + k) % NX
            start = ((to * NY + y) * NC + c) * DS + residue // RG * DB
            source = weight.at[at, pl.ds(pl.multiple_of(start, DB), DB)]
            target = plane_weights.at[residue, v, x]
            if k:
                remote(source, target, x_sems.at[2], x_sems.at[3], {"x": to}).start()
            else:
                pltpu.make_async_copy(source, target, local_sem.at[7]).start()
        return carry

    lax.fori_loop(1, NW, spread, 0)

    weights_to(1).wait_recv()
    weights_on(1).start()
    weights_to(3).wait_recv()
    weights_on(3).start()

    UP, DOWN = NW // 2, (NW - 1) // 2
    PIECES = ((3, 2, 1), (1, 2, 3))

    def chain(way, k, q):
        origin = (position + (NV * NW - k if way == 0 else k)) % (NV * NW)
        to = (up, down)[way]
        block = plane_weights.at[origin % NW, (to["v"] + q) % NV]
        return remote(block, block, chain_send.at[way, k, q], chain_recv.at[way, k, q], to)

    def start_chain():
        for qs in zip(*PIECES):
            for way, steps in enumerate((UP, DOWN)):
                if steps:
                    chain(way, 0, qs[way]).start()

    def pass_on(k):
        for qs in zip(*PIECES):
            for way, steps in enumerate((UP, DOWN)):
                if k < steps:
                    chain(way, k, qs[way]).wait_recv()
                if k + 1 < steps:
                    chain(way, k + 1, qs[way]).start()

    value_exchange = remote(values.at[own_half_rows], val_recv, pair_send.at[1], pair_recv.at[1], pair)
    value_exchange.start()

    half_exchange.wait_recv()
    value_grad_t = (own_half + half_recv[...].astype(F32)).astype(BF16)

    def core_copy(off):
        return remote(
            core_send.at[off],
            core_recv.at[off],
            core_ssem.at[off],
            core_rsem.at[off],
            {"c": 1 - c},
        )

    def make_blocks(turn, carry):
        off = (2 * turn + 1) % (NW + 1)
        to_w = (w + off % 2 * (beside - w) + off // 2 * 2) % NW
        for j in range(NY):
            block = (((y + j) % NY) * NW + to_w) * NC
            own = pl.multiple_of((block + c) * BD, BD)
            other = pl.multiple_of((block + 1 - c) * BD, BD)
            core_send[off, j] = dot(value_grad_t, hidden[:, pl.ds(other, BD)], 1, 0).astype(BF16)
            keep[off, j] = dot(value_grad_t, hidden[:, pl.ds(own, BD)], 1, 0)
        core_copy(off).start()
        return carry

    lax.fori_loop(0, NW, make_blocks, 0)

    quarter = half // 2

    def part_sum(off, j):
        return keep[off, j] + core_recv[off, j].astype(F32)

    def far_copy(off, way):
        at = pl.ds(way * quarter, quarter)
        return remote(
            far_send.at[off, at],
            far_recv.at[off, at],
            far_ssem,
            far_rsem.at[off],
            {"y": (y + (1, NY - 1)[way]) % NY},
        )

    def y_copy(off, way):
        return remote(
            y_send.at[off, way],
            y_recv.at[off, way],
            y_ssem,
            y_rsem.at[off],
            {"y": (y + (1, NY - 1)[way]) % NY},
        )

    def send_far(turn, carry):
        off = (2 * turn + 1) % (NW + 1)
        core_copy(off).wait_recv()
        far_send[off] = part_sum(off, 2).astype(BF16)
        far_copy(off, 0).start()
        far_copy(off, 1).start()
        return carry

    def send_y(turn, carry):
        off = (2 * turn + 1) % (NW + 1)
        wait_for(far_recv.at[off], far_rsem.at[off])
        came = far_recv[off].astype(F32)
        right, left = part_sum(off, 1), part_sum(off, 3)
        y_send[off, 0] = jnp.concatenate(
            [right[:quarter] + came[:quarter], right[quarter:]], axis=0
        ).astype(BF16)
        y_copy(off, 0).start()
        y_send[off, 1] = jnp.concatenate(
            [left[:quarter], left[quarter:] + came[quarter:]], axis=0
        ).astype(BF16)
        y_copy(off, 1).start()
        return carry

    lax.fori_loop(0, NW, send_far, 0)
    weights_on(1).wait_recv()
    weights_on(3).wait_recv()
    spread_blocks = plane_weights.at[pl.ds(0, NW - 1), 0, pl.ds(0, NX - 1)]
    wait_for(spread_blocks, x_sems.at[3])
    wait_for(plane_weights.at[pl.ds(0, NW - 1), 0, 0], local_sem.at[7])
    start_chain()

    lax.fori_loop(0, NW, send_y, 0)

    out_copy.wait()
    value_exchange.wait_recv()
    values[other_half_rows, :] = val_recv[...]
    key_part = jnp.zeros((width, T), F32)
    for h in range(heads):
        lanes = pl.ds(h * width, width)
        head_grad = grad[:, lanes]
        row_dots = jnp.sum(
            head_grad.astype(F32) * attn_out[:, lanes].astype(F32), axis=1, keepdims=True
        )
        prob_grad = dot(head_grad, values[...], 1, 0)
        score_grad = (probs[h] * (prob_grad - row_dots) * scale).astype(BF16)
        qgrad_ref[:, lanes] = dot(score_grad, keys[...], 1, 1).astype(BF16)
        key_part = key_part + dot(query[:, lanes], score_grad, 0, 0)
    own_kpart = jnp.where(lower, key_part[:half], key_part[half:])
    kpart_send[...] = jnp.where(lower, key_part[half:], key_part[:half]).astype(BF16)
    kpart_exchange = remote(kpart_send, kpart_recv, pair_send.at[3], pair_recv.at[3], pair)
    kpart_exchange.start()

    pass_on(0)

    for j in (1, 3, 2):
        part_to(j).wait_recv()
    own_tokens = jnp.concatenate(
        [
            part_recv[2 * i].astype(F32) + part_recv[2 * i + 1].astype(F32)
            for i in range(NV // 2)
        ],
        axis=1,
    )
    chips = NX * NY
    plane_grads[c, x * NY + y] = own_tokens.astype(BF16)

    def send_grads(i, carry):
        px, py = (x + i // NY) % NX, (y + i % NY) % NY
        block = plane_grads.at[c, x * NY + y]
        remote(block, block, plane_sems.at[0], plane_sems.at[1], {"x": px, "y": py}).start()
        return carry

    lax.fori_loop(1, chips, send_grads, 0)
    grads_over = remote(
        plane_grads.at[c], plane_grads.at[c], plane_sems.at[4], plane_sems.at[5], {"c": 1 - c}
    )

    def share_grads():
        wait_for(plane_grads.at[c, pl.ds(0, chips - 1)], plane_sems.at[1])
        grads_over.start()


    PAIRS = NW // 2

    def y_sum(off):
        wait_for(y_recv.at[off], y_rsem.at[off])
        return part_sum(off, 0) + y_recv[off, 0].astype(F32) + y_recv[off, 1].astype(F32)

    def w_copy(slot, step, to):
        return remote(
            w_send.at[slot], w_recv.at[slot], w_ssem, w_rsem.at[step], {"w": to}
        )

    for i in range(PAIRS):
        w_send[i] = y_sum(2 * i + 1).astype(BF16)
        w_copy(i, 0, beside).start()
    pass_on(1)
    wait_for(w_recv.at[pl.ds(0, PAIRS)], w_rsem.at[0])
    for i in range(1, PAIRS):
        w_send[PAIRS + i - 1] = (y_sum(2 * i) + w_recv[i].astype(F32)).astype(BF16)
        w_copy(PAIRS + i - 1, 1, (w + 2 * i) % NW).start()
    own_sum = y_sum(0) + w_recv[0].astype(F32)
    share_grads()
    for k in range(2, UP):
        pass_on(k)

    grads_over.wait_recv()
    NG = NY * NC
    pieces = []
    for d in range(2):
        acc = jnp.zeros((NG * TV, DB), F32)
        for i in range(NX):
            left = jnp.concatenate(
                [
                    plane_grads[k, i * NY : (i + 1) * NY].reshape(NY * TV, NV * half)
                    for k in range(NC)
                ],
                axis=0,
            )
            right = jnp.concatenate(
                [plane_weights[d * RG + g, k, i] for k in range(NV) for g in range(RG)], axis=0
            )
            acc = acc + dot(left, right, 1, 0)
        pieces.append(acc.reshape(NC, NY, NX, TR, DB))
    for i in range(NX):
        for j in range(NY):
            for k in range(NC):
                out_send[(i * NY + j) * NC + k] = jnp.concatenate(
                    [pieces[0][k, j, i], pieces[1][k, j, i]], axis=0
                ).astype(BF16)

    def send_out(i, carry):
        device, slot = plane(i)
        remote(
            out_send.at[slot], out_recv.at[me], plane_sems.at[2], plane_sems.at[3], device
        ).start()
        return carry

    lax.fori_loop(1, NS, send_out, 0)
    out_recv[me] = out_send[me]

    kpart_exchange.wait_recv()
    kgrad_ref[...] = (own_kpart + kpart_recv[...].astype(F32)).astype(BF16)
    wait_for(w_recv.at[pl.ds(PAIRS, PAIRS - 1)], w_rsem.at[1])
    summed = own_sum
    for i in range(PAIRS, NW - 1):
        summed = summed + w_recv[i].astype(F32)
    wgrad_ref[...] = summed
    wait_for(out_recv.at[pl.ds(0, NS - 1)], plane_sems.at[3])
    igrad_ref[...] = out_recv[...]

    for exchange in (key_exchange, value_exchange, half_exchange, kpart_exchange):
        exchange.wait_send()
    wait_for(plane_weights.at[w, v, pl.ds(0, NX - 1)], x_sems.at[0])
    for j in (1, 3):
        weights_to(j).wait_send()
        weights_on(j).wait_send()
    for j in (1, 2, 3):
        part_to(j).wait_send()
    wait_for(spread_blocks, x_sems.at[2])
    for way, steps in enumerate((UP, DOWN)):
        for k in range(steps):
            for q in PIECES[way]:
                chain(way, k, q).wait_send()

    def core_sent(off, carry):
        core_copy(off).wait_send()
        return carry

    lax.fori_loop(0, NW, core_sent, 0)
    wait_for(far_send, far_ssem)
    wait_for(y_send, y_ssem)
    wait_for(w_send, w_ssem)
    wait_for(plane_grads.at[c, pl.ds(0, chips - 1)], plane_sems.at[0])
    grads_over.wait_send()
    wait_for(out_send.at[pl.ds(0, NS - 1)], plane_sems.at[2])


def hand_over(*refs):
    sems = refs[-1]
    copies = [
        pltpu.make_async_copy(source, target, sems.at[i])
        for i, (source, target) in enumerate(zip(refs[:4], refs[4:8]))
    ]
    for copy in copies:
        copy.start()
    for copy in copies:
        copy.wait()


def per_device(
    sizes,
    hidden_in,
    value_weight,
    queries,
    key_rows,
    attention_out,
    output_grad,
    log_normalizer,
    document_ids,
):
    NX, NY, NW, NC, NV = sizes
    T, D = hidden_in.shape[1:]
    half = key_rows.shape[2]
    width = 2 * half
    heads = log_normalizer.shape[2]
    NS = NX * NY * NC
    DS = D // NS
    DB = DS // 2
    R = half // (NW // 2)
    TR = T // (NX * NV)
    TV = T // NV
    BD = D // (NY * NW * NC)
    half_block = pltpu.VMEM((half, T), BF16)
    dma = pltpu.SemaphoreType.DMA
    scratch = [
        pltpu.VMEM((heads, T), F32),
        pltpu.VMEM((1, T), jnp.int32),
        pltpu.VMEM((T, D), BF16),
        pltpu.VMEM((half, D), BF16),
        pltpu.VMEM((NX, R, DB), BF16),
        pltpu.VMEM((T, heads * width), BF16),
        pltpu.VMEM((T, heads * width), BF16),
        pltpu.VMEM((T, heads * width), BF16),
        half_block,
        half_block,
        pltpu.VMEM((width, T), BF16),
        pltpu.VMEM((width, T), BF16),
        pltpu.VMEM((heads, T, T), F32),
        half_block,
        half_block,
        half_block,
        half_block,
        pltpu.VMEM((NV, TV, width), BF16),
        pltpu.VMEM((NV, TV, width), BF16),
        pltpu.VMEM((NC, NX * NY, TV, NV * half), BF16),
        pltpu.VMEM((NW, NV, NX, R, DB), BF16),
        pltpu.VMEM((NS, 2 * TR, DB), BF16),
        pltpu.VMEM((NS, 2 * TR, DB), BF16),
        pltpu.VMEM((NW, NY, half, BD), F32),
        pltpu.VMEM((NW, NY, half, BD), BF16),
        pltpu.VMEM((NW, NY, half, BD), BF16),
        pltpu.VMEM((NW, half, BD), BF16),
        pltpu.VMEM((NW, half, BD), BF16),
        pltpu.VMEM((NW, 2, half, BD), BF16),
        pltpu.VMEM((NW, 2, half, BD), BF16),
        pltpu.VMEM((NW - 1, half, BD), BF16),
        pltpu.VMEM((NW - 1, half, BD), BF16),
        dma((8,)),
        dma((4,)),
        dma((NX,)),
        dma((4,)),
        dma((4,)),
        dma((4,)),
        dma((NV,)),
        dma((NV,)),
        dma((NV,)),
        dma((NV,)),
        dma((2, NW // 2, NV)),
        dma((2, NW // 2, NV)),
        dma((6,)),
        dma((NW,)),
        dma((NW,)),
        dma,
        dma((NW,)),
        dma,
        dma((NW,)),
        dma,
        dma((2,)),
    ]
    anywhere = pl.BlockSpec(memory_space=pltpu.HBM)
    vmem = pl.BlockSpec(memory_space=pltpu.VMEM)
    results = pl.pallas_call(
        functools.partial(kernel, sizes),
        out_shape=(
            jax.ShapeDtypeStruct((T, heads * width), BF16),
            jax.ShapeDtypeStruct((half, T), BF16),
            jax.ShapeDtypeStruct((NS, 2 * TR, DB), BF16),
            jax.ShapeDtypeStruct((half, BD), F32),
        ),
        in_specs=[anywhere] * 8,
        out_specs=(vmem,) * 4,
        scratch_shapes=scratch,
        compiler_params=pltpu.CompilerParams(
            collective_id=0, has_side_effects=True, vmem_limit_bytes=48 * 1024 * 1024
        ),
    )(
        *(
            pltpu.with_memory_space_constraint(array, pltpu.HBM)
            for array in (
                hidden_in[0],
                value_weight.T,
                queries[0],
                key_rows[0].T,
                attention_out[0],
                output_grad[0],
                log_normalizer[0].T,
                document_ids,
            )
        )
    )
    query_grad, key_grad, input_blocks, weight_grad = pl.pallas_call(
        hand_over,
        out_shape=tuple(jax.ShapeDtypeStruct(r.shape, r.dtype) for r in results),
        in_specs=(vmem,) * 4,
        out_specs=(anywhere,) * 4,
        scratch_shapes=[dma((4,))],
        compiler_params=pltpu.CompilerParams(vmem_limit_bytes=8 * 1024 * 1024),
    )(*results)
    input_grad = (
        input_blocks.reshape(NS, 2, TR, DB).transpose(2, 0, 1, 3).reshape(1, TR, D)
    )
    return query_grad[None], key_grad.T[None], input_grad, weight_grad.T


def over(finer):
    sizes = tuple(finer.shape[name] for name in ("x", "y", "w", "c", "v"))
    return jax.shard_map(
        functools.partial(per_device, sizes),
        mesh=finer,
        in_specs=(
            P(DP, None, None),
            P(None, TENSOR),
            P(DP, None, TENSOR),
            P(DP, None, TENSOR),
            P(DP, None, TENSOR),
            P(DP, None, TENSOR),
            P(DP, None, TENSOR),
            P(DP, None),
        ),
        out_specs=(P(DP, None, TENSOR), P(DP, None, TENSOR), P(DP, TENSOR, None), P(DP, TENSOR)),
        check_vma=False,
    )


def solution(mesh):
    return over(Mesh(mesh.devices.reshape(4, 8, 2, 4, 4), DP + TENSOR))
```
